256 devices in a mesh: blk: 128 (over z, x, y), fld: 2 (over core).
Axes of the slice: x: 4, y: 4, z: 8, core: 2. Of those that a mesh axis runs over, the one named last changes fastest.
Arguments:
- seed_fine: float32 [8, 1024, 4096], P('fld', 'blk'), may hold values from -6 to 6
- seed_coarse: float32 [8, 256, 4096], P('fld', 'blk'), may hold values from -6 to 6
- saved_fine: float32 [4, 8, 1024, 4096], P(None, 'fld', 'blk'), may hold values from 0.5 to 2
- saved_coarse: float32 [2, 8, 256, 4096], P(None, 'fld', 'blk'), may hold values from 0.5 to 2
- diffusion: float32 [8], P('fld'), may hold values from 0.02 to 0.15
- species_shares: float32 [8], P('fld'), may hold values from 0.1 to 1
- fine_nbr: int32 [1024, 6], P('blk'), may hold values from -1 to 1023, as said below
- coarse_nbr: int32 [256, 6], P('blk'), may hold values from -1 to 255, as said below
- children: int32 [256, 8], P('blk'), may hold values from -1 to 1023, as said below
- fine_counts: int32 [1024], P('blk'), may hold values from 1 to 4
- coarse_counts: int32 [256], P('blk'), may hold values from 1 to 4
Outputs:
- adj_fine: float32 [8, 1024, 4096], P('fld', 'blk')
- adj_coarse: float32 [8, 256, 4096], P('fld', 'blk')
The draws below stay inside these ranges and needn't reach their ends.
Inputs may be any that keep to these rules, and one draw needn't show every extreme that they name: `fine_nbr`: slot of the block beside each face (first and last along cell dimensions 0, 1, 2), -1 at a wall. The relation is symmetric with faces 2a and 2a+1 paired. Across faces 0 to 3 the neighbour is held by the same index of blk, across face 4 by the same or the one below, across face 5 by the same or the one above. `coarse_nbr`: as for the fine level: symmetric, faces 2a and 2a+1 paired; across faces 0 to 3 the same index of blk, across face 4 the same or the one below, across face 5 the same or the one above. `children`: the fine block that refines each coarse octant, or -1. Every fine block refines exactly one octant. The octants held by index i of blk that are refined are refined by blocks of the indices i + d modulo 128 for d = 0 .. 7, exactly 1 of them by the blocks of each such index.
All inputs are finite; a program needn't handle non-finite values.
Results may differ from the reference program's by a relative error of at most 0.0003.
Values sent between devices are 32-bit elements; how exact they have to be, the bound alone decides.
A program may use at most 128 MiB of HBM per device.

```python
import math
import jax
import jax.numpy as jnp

NV = 8
B = 16
LX = 2
LY = 2
FZ = 2
NSUB = 4
CYCLES = 2
BF = 8
BC = 2
NF = 1024
NC = 256


def lattice_neighbours(key, span_x, span_y, span_z, devices):
    per_dev = span_x * span_y * span_z
    subkeys = jax.random.split(key, devices)
    orders = jax.vmap(lambda subkey: jax.random.permutation(subkey, per_dev))(subkeys).astype(jnp.int32)
    slot_of = (jnp.arange(devices, dtype=jnp.int32)[:, None] * per_dev + orders).reshape(-1)
    logical = jnp.arange(devices * per_dev, dtype=jnp.int32)
    device_no = logical // per_dev
    local_no = logical % per_dev
    pos_x = local_no // (span_y * span_z)
    pos_y = local_no // span_z % span_y
    pos_z = device_no * span_z + local_no % span_z
    full_depth = devices * span_z
    columns = []
    for axis_no in range(3):
        for direction in (-1, 1):
            shifted = [pos_x, pos_y, pos_z]
            shifted[axis_no] = shifted[axis_no] + direction
            upper_end = (span_x, span_y, full_depth)[axis_no]
            inside = (shifted[axis_no] >= 0) & (shifted[axis_no] < upper_end)
            target = shifted[2] // span_z * per_dev + (shifted[0] * span_y + shifted[1]) * span_z + shifted[2] % span_z
            target = jnp.clip(target, 0, devices * per_dev - 1)
            columns.append(jnp.where(inside, slot_of[target], -1))
    neighbour_table = jnp.stack(columns, axis=1).astype(jnp.int32)
    return jnp.zeros((devices * per_dev, 6), jnp.int32).at[slot_of].set(neighbour_table)


def draw_fine_nbr(key, part):
    return lattice_neighbours(jax.random.fold_in(key, 11), LX, LY, FZ, NF // BF)


def draw_coarse_nbr(key, part):
    return lattice_neighbours(jax.random.fold_in(key, 23), LX // 2, LY, FZ // 2, NC // BC)


def draw_children(key, part):
    devices = NF // BF
    links = min(BF, devices)
    per_link = BF // links
    octant_count = 8 * BC
    subkeys = jax.random.split(jax.random.fold_in(key, 37), 2)
    fine_orders = jax.vmap(lambda subkey: jax.random.permutation(subkey, BF))(jax.random.split(subkeys[0], devices)).astype(jnp.int32)
    coarse_orders = jax.vmap(lambda subkey: jax.random.permutation(subkey, octant_count))(jax.random.split(subkeys[1], devices)).astype(jnp.int32)
    holder = jnp.arange(devices, dtype=jnp.int32)[:, None, None]
    link_no = jnp.arange(links, dtype=jnp.int32)[None, :, None]
    member = jnp.arange(per_link, dtype=jnp.int32)[None, None, :]
    position = link_no * per_link + member
    source = (holder + link_no) % devices
    fine_ids = source * BF + fine_orders[source, position]
    octant_ids = holder * octant_count + coarse_orders[holder, position]
    fine_ids = jnp.broadcast_to(fine_ids, (devices, links, per_link)).reshape(-1)
    octant_ids = jnp.broadcast_to(octant_ids, (devices, links, per_link)).reshape(-1)
    flat_child = jnp.full((devices * octant_count,), -1, jnp.int32).at[octant_ids].set(fine_ids.astype(jnp.int32))
    return flat_child.reshape(NC, 8)


def touch_ends(array, key, smallest, high):
    shape = array.shape
    spot = [jax.random.randint(jax.random.fold_in(key, axis), (), 0, shape[axis]) for axis in range(len(shape))]
    array = array.at[tuple(spot)].set(smallest)
    longest = shape.index(max(shape))
    spot[longest] = (spot[longest] + 1) % shape[longest]
    return array.at[tuple(spot)].set(high)


def levels(stream_key, shape, pieces, low, top_value):
    def one(dim, parts):
        steps = jax.random.uniform(jax.random.fold_in(jax.random.fold_in(stream_key, 6), dim), (parts,), jnp.float32, low / len(pieces), top_value / len(pieces))
        return jnp.repeat(jnp.exp(steps), shape[dim] // parts).reshape((-1,) + (1,) * (len(shape) - dim - 1))

    factor_of = one(*pieces[0])
    for cut in pieces[1:]:
        factor_of = factor_of * one(*cut)
    return factor_of


def normal_values(stream_key, extent, scale, bound, shards=(), kind=jnp.bfloat16):
    entries = jax.random.normal(stream_key, extent, jnp.float32) * scale
    if len(shards) > 0:
        entries = levels(stream_key, extent, shards, -0.22, 0.18) * entries
    return jnp.clip(entries, min=-bound, max=bound).astype(kind)


def setup_inputs(seed: int = 0) -> dict:
    key_of = jax.random.split(jax.random.key(seed), 12)
    seed_fine = normal_values(key_of[0], (NV, NF, B**3), 1.0, 6.0, ((0, 2), (1, 128)), jnp.float32)
    seed_coarse = normal_values(key_of[1], (NV, NC, B**3), 1.0, 6.0, ((0, 2), (1, 128)), jnp.float32)
    saved_fine = jnp.clip(0.5 + 1.5 * jax.random.uniform(key_of[2], (2 * CYCLES, NV, NF, B**3), jnp.float32) ** levels(key_of[2], (2 * CYCLES, NV, NF, B**3), ((1, 2), (2, 128)), -0.2, 0.2), 0.5, 2.0)
    saved_coarse = jnp.clip(0.5 + 1.5 * jax.random.uniform(key_of[3], (CYCLES, NV, NC, B**3), jnp.float32) ** levels(key_of[3], (CYCLES, NV, NC, B**3), ((1, 2), (2, 128)), -0.2, 0.2), 0.5, 2.0)
    diffusion = jnp.clip(jnp.exp(math.log(0.15) - 2.014903 * jax.random.uniform(key_of[4], (NV,), jnp.float32) ** levels(key_of[4], (NV,), ((0, 2),), -0.2, 0.2)), 0.02, 0.15)
    species_shares = jnp.clip(jnp.exp(math.log(1.0) - 2.3025851 * jax.random.uniform(key_of[5], (NV,), jnp.float32) ** levels(key_of[5], (NV,), ((0, 2),), -0.2, 0.2)), 0.1, 1.0)
    fine_nbr = draw_fine_nbr(jax.random.fold_in(key_of[11], 71), 0)
    coarse_nbr = draw_coarse_nbr(jax.random.fold_in(key_of[11], 71), 0)
    children = draw_children(jax.random.fold_in(key_of[11], 71), 0)
    fine_counts = touch_ends(jax.random.randint(key_of[9], (NF,), 1, NSUB + 1), jax.random.fold_in(key_of[9], 1), 1, NSUB).astype(jnp.int32)
    coarse_counts = touch_ends(jax.random.randint(key_of[10], (NC,), 1, NSUB + 1), jax.random.fold_in(key_of[10], 1), 1, NSUB).astype(jnp.int32)
    return dict(seed_fine=seed_fine, seed_coarse=seed_coarse, saved_fine=saved_fine, saved_coarse=saved_coarse, diffusion=diffusion, species_shares=species_shares, fine_nbr=fine_nbr, coarse_nbr=coarse_nbr, children=children, fine_counts=fine_counts, coarse_counts=coarse_counts)


heat_gain = 0.5
energy = 2.0


def face_list(field):
    return [field[:, :, 0], field[:, :, -1], field[:, :, :, 0], field[:, :, :, -1], field[:, :, :, :, 0], field[:, :, :, :, -1]]


def with_ghosts(field, ghosts):
    running = -6.0 * field
    running = running + jnp.concatenate([ghosts[0][:, :, None], field[:, :, :-1]], axis=2)
    running = running + jnp.concatenate([field[:, :, 1:], ghosts[1][:, :, None]], axis=2)
    running = running + jnp.concatenate([ghosts[2][:, :, :, None], field[:, :, :, :-1]], axis=3)
    running = running + jnp.concatenate([field[:, :, :, 1:], ghosts[3][:, :, :, None]], axis=3)
    running = running + jnp.concatenate([ghosts[4][..., None], field[..., :-1]], axis=4)
    running = running + jnp.concatenate([field[..., 1:], ghosts[5][..., None]], axis=4)
    return running


def laplace(field, neighbours):
    faces = face_list(field)
    ghosts = []
    for face_no in range(6):
        target = neighbours[:, face_no]
        chosen = faces[face_no ^ 1][:, jnp.maximum(target, 0)]
        ghosts.append(jnp.where((target >= 0)[None, :, None, None], chosen, jnp.zeros_like(chosen)))
    return with_ghosts(field, ghosts)


def diffuse_adjoint(costate_values, neighbours, rates):
    first = rates * laplace(costate_values, neighbours)
    second = rates * laplace(first, neighbours)
    return costate_values + first + 0.5 * second


def exothermic_sources(thermal_costate, thermal_profile, tally_grid, blend_aggregate):
    substep = 1.0 / tally_grid.astype(jnp.float32)[:, None]
    history = []
    present_refinement = thermal_profile
    for counter in range(NSUB):
        history.append(present_refinement)
        active = (counter < tally_grid)[:, None]
        present_refinement = present_refinement + jnp.where(active, substep * heat_gain * blend_aggregate * jnp.exp(-energy / present_refinement), 0.0)
    remainder_passed = thermal_costate
    scaling_coefficient = jnp.zeros_like(thermal_costate)
    for counter in reversed(range(NSUB)):
        earlier = history[counter]
        active = (counter < tally_grid)[:, None]
        decay = jnp.exp(-energy / earlier)
        scaling_coefficient = scaling_coefficient + jnp.where(active, substep * heat_gain * decay * remainder_passed, 0.0)
        remainder_passed = jnp.where(active, remainder_passed * (1.0 + substep * heat_gain * blend_aggregate * energy * decay / (earlier * earlier)), remainder_passed)
    return remainder_passed, scaling_coefficient


def reaction_adjoint(costate_values, saved, tally_grid, species_shares):
    blend_aggregate = jnp.sum(species_shares[:, None, None] * saved, axis=0)
    remainder_passed, scaling_coefficient = exothermic_sources(costate_values[0], saved[0], tally_grid, blend_aggregate)
    costate_values = jnp.concatenate([remainder_passed[None], costate_values[1:]], axis=0)
    return costate_values + species_shares[:, None, None] * scaling_coefficient[None]


def restrict_adjoint(fine_adj, coarse_adj, children):
    fields = fine_adj.shape[0]
    count_c = coarse_adj.shape[1]
    half_edge = B // 2
    octants = coarse_adj.reshape(fields, count_c, 2, half_edge, 2, half_edge, 2, half_edge)
    octants = octants.transpose(0, 1, 2, 4, 6, 3, 5, 7).reshape(fields, count_c * 8, half_edge, half_edge, half_edge)
    flat_child = children.reshape(-1)
    refined = jnp.nonzero(flat_child >= 0, size=NF)[0].astype(jnp.int32)
    fine_ids = flat_child[refined].astype(jnp.int32)
    portion = octants[:, refined] * 0.125
    portion = jnp.repeat(jnp.repeat(jnp.repeat(portion, 2, axis=2), 2, axis=3), 2, axis=4)
    fine_adj = fine_adj.at[:, fine_ids].add(portion)
    keeping = (flat_child < 0).astype(coarse_adj.dtype).reshape(count_c, 2, 2, 2)
    shaped = coarse_adj.reshape(fields, count_c, 2, half_edge, 2, half_edge, 2, half_edge)
    coarse_adj = (shaped * keeping[None, :, :, None, :, None, :, None]).reshape(coarse_adj.shape)
    return fine_adj, coarse_adj


def reference(seed_fine, seed_coarse, saved_fine, saved_coarse, diffusion, species_shares, fine_nbr, coarse_nbr, children, fine_counts, coarse_counts):
    cell_count = B ** 3
    fine_adj = seed_fine.reshape(NV, NF, B, B, B)
    coarse_adj = seed_coarse.reshape(NV, NC, B, B, B)
    fine_rates = diffusion.reshape(NV, 1, 1, 1, 1)
    coarse_rates = 0.5 * fine_rates
    for sweep_no in reversed(range(CYCLES)):
        fine_adj, coarse_adj = restrict_adjoint(fine_adj, coarse_adj, children)
        for stepno in (2 * sweep_no + 1, 2 * sweep_no):
            flat_fine = reaction_adjoint(fine_adj.reshape(NV, NF, cell_count), saved_fine[stepno], fine_counts, species_shares)
            fine_adj = diffuse_adjoint(flat_fine.reshape(NV, NF, B, B, B), fine_nbr, fine_rates)
        flat_coarse = reaction_adjoint(coarse_adj.reshape(NV, NC, cell_count), saved_coarse[sweep_no], coarse_counts, species_shares)
        coarse_adj = diffuse_adjoint(flat_coarse.reshape(NV, NC, B, B, B), coarse_nbr, coarse_rates)
    return fine_adj.reshape(NV, NF, cell_count), coarse_adj.reshape(NV, NC, cell_count)
```

```python
import functools

import jax
import jax.numpy as jnp
from jax import lax
from jax.experimental import pallas as pl
from jax.experimental.pallas import tpu as pltpu
from jax.sharding import PartitionSpec as P

NSUB = 4
FIELDS = 4
ROWS = 8
LANES = 128
TILES = 32
LINKS = 8
COARSE = FIELDS
HEAT = 0.5
ENERGY = 2.0


def rows_of(x, idx):
    return jnp.take_along_axis(x, idx, axis=0, mode="promise_in_bounds")


def lanes_of(x, idx):
    return jnp.take_along_axis(x, idx, axis=1, mode="promise_in_bounds")


def lane_roll(x, steps):
    steps = steps % LANES
    return x if steps == 0 else pltpu.roll(x, steps, 1)


def row_roll(x, steps):
    return pltpu.roll(x, steps % ROWS, 0)


def kernel(
    n,
    seed_fine, seed_coarse, saved_fine, saved_coarse, diffusion, shares, fine_nbr, coarse_nbr, children,
    fine_counts, coarse_counts,
    out_fine, out_coarse,
    X, FL, FF, GG, PM, MR, W, HS, HR, RS, RR, NI, NL, NR, RT, SH, FM, KM, HN, CN, OC,
    h_send, h_recv, w_send, w_recv, m_send, m_recv, r_send, r_recv,
):
    me = lax.axis_index("blk")
    fld = lax.axis_index("fld")
    partner = {"fld": 1 - fld}

    def at(d):
        return {"blk": lax.rem(me + (d + n), n)}

    barrier = pltpu.get_barrier_semaphore()
    pl.semaphore_signal(barrier, inc=1, device_id=partner, device_id_type=pl.DeviceIdType.MESH)
    for d in range(1, LINKS):
        for way in (d, -d):
            pl.semaphore_signal(barrier, inc=1, device_id=at(way), device_id_type=pl.DeviceIdType.MESH)

    shape = (ROWS, LANES)
    row = lax.broadcasted_iota(jnp.int32, shape, 0)
    lane = lax.broadcasted_iota(jnp.int32, shape, 1)
    kk = lane & 15
    even = (row & 1) == 0
    zero = jnp.zeros(shape, jnp.float32)

    def cols(q):
        return pl.ds(pl.multiple_of(q * LANES, LANES), LANES)

    def spread_rows(values):
        out = jnp.full(shape, values[0])
        for r in range(1, ROWS):
            out = jnp.where(row == r, values[r], out)
        return out

    for f in range(FIELDS):
        RT[f] = jnp.full(shape, diffusion[f])
        SH[f] = jnp.full(shape, shares[f])
        FM[f] = jnp.full(shape, jnp.where((fld == 0) & (f == 0), 1.0, 0.0))
    RT[COARSE] = spread_rows([0.5 * diffusion[r // 2] for r in range(ROWS)])
    SH[COARSE] = spread_rows([shares[r // 2] for r in range(ROWS)])
    FM[COARSE] = jnp.where((row < 2) & (fld == 0), 1.0, 0.0)
    CN[0] = spread_rows([fine_counts[r] for r in range(ROWS)])
    CN[1] = spread_rows([coarse_counts[r % 2] for r in range(ROWS)])
    for level in range(2):
        HN[level] = 1.0 / CN[level].astype(jnp.float32)
        for face in range(6):
            if level == 0:
                raw = spread_rows([fine_nbr[r, face] for r in range(ROWS)])
                base, per, idx = me * 8, 8, raw & 7
            else:
                raw = spread_rows([coarse_nbr[r % 2, face] for r in range(ROWS)])
                base, per, idx = me * 2, 2, (row & 6) + (raw & 1)
            there = raw >= 0
            local = there & (raw >= base) & (raw < base + per)
            NI[level * 6 + face] = idx
            NL[level * 6 + face] = jnp.where(local, 1, 0)
            if face >= 4:
                NR[level * 2 + face - 4] = jnp.where(there & ~local, 1, 0)

    for d in range(LINKS):
        octant, slot = jnp.int32(0), jnp.int32(0)
        for p in range(2):
            for o in range(8):
                child = children[p, o]
                hit = (child >= 0) & ((((child >> 3) - me) & (n - 1)) == d)
                octant = jnp.where(hit, p * 8 + o, octant)
                slot = jnp.where(hit, child & 7, slot)
        OC[d] = octant
        OC[LINKS + d] = slot
    keep = [[jnp.where(children[p, o] < 0, 1.0, 0.0) for o in range(8)] for p in range(2)]
    for ab in range(4):
        halves = [jnp.where(kk < 8, keep[p][2 * ab], keep[p][2 * ab + 1]) for p in range(2)]
        KM[ab] = jnp.where(even, halves[0], halves[1])

    def load_coarse(q, _):
        for f in range(FIELDS):
            X[COARSE, q, 2 * f : 2 * f + 2, :] = seed_coarse[f, :, cols(q)]
        return 0

    lax.fori_loop(0, TILES, load_coarse, 0, unroll=4)

    pl.semaphore_wait(barrier, 2 * (LINKS - 1) + 1)

    def octant_copy(rslot, d):
        return pltpu.make_async_remote_copy(
            src_ref=RS.at[rslot, d], dst_ref=RR.at[rslot, d], send_sem=r_send.at[rslot, d],
            recv_sem=r_recv.at[rslot, d], device_id=at(d), device_id_type=pl.DeviceIdType.MESH,
        )

    def send_octants(rslot):
        for d in (7, 6, 5, 4, 3, 2, 1, 0):
            octant = OC[d]
            p, a, b, c = octant >> 3, (octant >> 2) & 1, (octant >> 1) & 1, octant & 1
            parts = []
            for i in range(8):
                v = X[COARSE, (a * 8 + i) * 2 + b]
                v = jnp.where(jnp.full(shape, c) == 1, lane_roll(v, -8), v)
                v = jnp.where(jnp.full(shape, p) == 1, row_roll(v, -1), v)
                parts.append(v)
            target = RR if d == 0 else RS
            for u in range(2):
                pair = []
                for g in range(2):
                    at_i = u * 4 + g * 2
                    pair.append(jnp.where(kk < 8, parts[at_i], lane_roll(parts[at_i + 1], 8)))
                target[rslot, d, u] = jnp.where(even, pair[0], row_roll(pair[1], 1))
            target[rslot, d, 2] = jnp.full(shape, OC[LINKS + d]).astype(jnp.float32)
            if d:
                octant_copy(rslot, d).start()

    def mask_coarse():
        def one(i, _):
            for b in range(2):
                X[COARSE, i * 2 + b] = X[COARSE, i * 2 + b] * KM[(i >> 3) * 2 + b]
            return 0

        lax.fori_loop(0, 16, one, 0, unroll=4)

    def wait_octants(rslot):
        for d in range(1, LINKS):
            octant_copy(rslot, d).wait_recv()

    spread_idx = [
        [((lane >> 5) + jh * 4) * 16 + h * 8 + ((lane & 15) >> 1) for jh in range(2)] for h in range(2)
    ]

    def add_octants(rslot, f, source):
        mine = [RR[rslot, d, 2] == row.astype(jnp.float32) for d in range(LINKS)]
        for u in range(2):
            for g in range(2):
                total = zero
                for d in range(LINKS):
                    line = jnp.broadcast_to(RR[rslot, d, u, pl.ds(f * 2 + g, 1), :], shape)
                    total = jnp.where(mine[d], line, total)
                total = 0.125 * total
                for h in range(2):
                    i = (u * 4 + g * 2 + h) * 2
                    for jh in range(2):
                        gain = lanes_of(total, spread_idx[h][jh])
                        for q in (i * 2 + jh, (i + 1) * 2 + jh):
                            X[f, q] = source(q) + gain

    def mix_copy(slot):
        return pltpu.make_async_remote_copy(
            src_ref=PM.at[slot], dst_ref=MR.at[slot], send_sem=m_send.at[slot], recv_sem=m_recv.at[slot],
            device_id=partner, device_id_type=pl.DeviceIdType.MESH,
        )

    def part_fine(s):
        def one(q, _):
            total = SH[0] * saved_fine[3 - s, 0, :, cols(q)]
            for f in range(1, FIELDS):
                total = total + SH[f] * saved_fine[3 - s, f, :, cols(q)]
            PM[s, q] = total
            return 0

        lax.fori_loop(0, TILES, one, 0, unroll=4)

    def coarse_rows(c, f, q):
        first = jnp.broadcast_to(saved_coarse[c, f, 0:1, cols(q)], shape)
        return jnp.where(even, first, jnp.broadcast_to(saved_coarse[c, f, 1:2, cols(q)], shape))

    def part_coarse(s):
        def one(q, _):
            total = SH[0] * coarse_rows(1 - s, 0, q)
            for f in range(1, FIELDS):
                total = total + SH[f] * coarse_rows(1 - s, f, q)
            PM[4 + s, q] = total
            return 0

        lax.fori_loop(0, TILES, one, 0, unroll=4)

    def factors(slot, level, temperature):
        mix_copy(slot).wait_recv()

        def one(q, _):
            count = CN[level]
            half = HN[level] * HEAT
            mix = PM[slot, q] + MR[slot, q]
            t = temperature(q)
            saved = []
            for k in range(NSUB):
                inverse = 1.0 / t
                e = half * jnp.exp(-ENERGY * inverse)
                saved.append((inverse, e))
                if k + 1 < NSUB:
                    t = jnp.where(k < count, t + mix * e, t)
            f, g = jnp.ones(shape, jnp.float32), zero
            for k in reversed(range(NSUB)):
                inverse, e = saved[k]
                live = k < count
                g = jnp.where(live, g + e * f, g)
                f = jnp.where(live, f + f * (ENERGY * mix * e * (inverse * inverse)), f)
            FF[slot, q] = f
            GG[slot, q] = g
            return 0

        lax.fori_loop(0, TILES, one, 0, unroll=4)

    def factors_fine(s):
        factors(s, 0, lambda q: saved_fine[3 - s, 0, :, cols(q)])

    def factors_coarse(s):
        factors(4 + s, 1, lambda q: coarse_rows(1 - s, 0, q))

    def w_copy(slot):
        return pltpu.make_async_remote_copy(
            src_ref=W.at[slot], dst_ref=W.at[slot], send_sem=w_send.at[slot], recv_sem=w_recv.at[slot],
            device_id=partner, device_id_type=pl.DeviceIdType.MESH,
        )

    def weights(slot, f, level):
        @pl.when(fld == 0)
        def _():
            source = jnp.where(jnp.full(shape, level) == 1, row & 1, row)

            def one(q, _):
                W[slot, q] = GG[slot, q] * rows_of(X[f, q], source)
                return 0

            lax.fori_loop(0, TILES, one, 0, unroll=8)
            w_copy(slot).start()

        @pl.when(fld == 1)
        def _():
            w_copy(slot).wait_recv()

    def halo_copy(slot, way):
        return pltpu.make_async_remote_copy(
            src_ref=HS.at[slot, way], dst_ref=HR.at[slot, way], send_sem=h_send.at[slot, way],
            recv_sem=h_recv.at[slot, way], device_id=at(1 if way == 0 else -1),
            device_id_type=pl.DeviceIdType.MESH,
        )

    def laplace(v, level, g4, g5, emit):
        idx = [NI[level * 6 + face] for face in range(4)]
        has = [NL[level * 6 + face] > 0 for face in range(4)]

        def ghost(x, face):
            return jnp.where(has[face], rows_of(x, idx[face]), zero)

        for i in range(16):
            pair = [v(2 * i), v(2 * i + 1)]
            up = [lane_roll(x, 16) for x in pair]
            down = [lane_roll(x, -16) for x in pair]
            j_less = [jnp.where(lane < 16, ghost(up[1], 2), up[0]), jnp.where(lane < 16, up[0], up[1])]
            j_more = [
                jnp.where(lane >= 112, down[1], down[0]),
                jnp.where(lane >= 112, ghost(down[0], 3), down[1]),
            ]
            for jh in range(2):
                q = 2 * i + jh
                u, m = q // 16, q % 16
                x = pair[jh]
                i_less = v(q - 2) if i > 0 else ghost(v(30 + jh), 0)
                i_more = v(q + 2) if i < 15 else ghost(v(jh), 1)
                k_less = jnp.where(kk == 0, lane_roll(g4[u], -m), lane_roll(x, 1))
                k_more = jnp.where(kk == 15, lane_roll(g5[u], 15 - m), lane_roll(x, -1))
                total = ((i_less + i_more) + (j_less[jh] + j_more[jh])) + ((k_less + k_more) - 6.0 * x)
                emit(q, x, total)

    def pack(v, k):
        packed = []
        for u in range(2):
            out = zero
            for m in range(16):
                out = jnp.where(kk == m, lane_roll(v(u * 16 + m), m - k), out)
            packed.append(out)
        return packed

    def begin(s, f, level):
        slot = s * 5 + f
        wslot = level * 4 + s
        rate = RT[f]
        share = SH[f]
        scaled = FM[f] > 0

        for q in range(TILES):
            X[f, q] = X[f, q] * jnp.where(scaled, FF[wslot, q], 1.0) + share * W[wslot, q]
        low = pack(lambda q: X[f, q], 0)
        high = pack(lambda q: X[f, q], 15)
        idx4, idx5 = NI[level * 6 + 4], NI[level * 6 + 5]
        has4, has5 = NL[level * 6 + 4] > 0, NL[level * 6 + 5] > 0
        g4 = [jnp.where(has4, rows_of(x, idx4), zero) for x in high]
        g5 = [jnp.where(has5, rows_of(x, idx5), zero) for x in low]

        def emit(q, x, total):
            FL[f, q] = rate * total

        laplace(lambda q: X[f, q], level, g4, g5, emit)
        low_first = pack(lambda q: FL[f, q], 0)
        high_first = pack(lambda q: FL[f, q], 15)
        for u in range(2):
            HS[slot, 0, u] = high[u]
            HS[slot, 0, 2 + u] = high_first[u]
            HS[slot, 1, u] = low[u]
            HS[slot, 1, 2 + u] = low_first[u]
        halo_copy(slot, 0).start()
        halo_copy(slot, 1).start()

    def finish(s, f, level):
        slot = s * 5 + f
        rate = RT[f]
        halo_copy(slot, 0).wait_recv()
        halo_copy(slot, 1).wait_recv()
        idx4, idx5 = NI[level * 6 + 4], NI[level * 6 + 5]
        has4, has5 = NL[level * 6 + 4] > 0, NL[level * 6 + 5] > 0
        far4, far5 = NR[level * 2] > 0, NR[level * 2 + 1] > 0
        r4, r5, g4, g5 = [], [], [], []
        for u in range(2):
            r4.append(jnp.where(far4, rate * rows_of(HR[slot, 0, u], idx4), zero))
            r5.append(jnp.where(far5, rate * rows_of(HR[slot, 1, u], idx5), zero))
        for u in range(2):
            low_first = HS[slot, 1, 2 + u] + r4[u]
            high_first = HS[slot, 0, 2 + u] + r5[u]
            far_low = rows_of(HR[slot, 0, 2 + u], idx4) + rate * HS[slot, 1, u]
            far_high = rows_of(HR[slot, 1, 2 + u], idx5) + rate * HS[slot, 0, u]
            g4.append(jnp.where(has4, rows_of(high_first, idx4), jnp.where(far4, far_low, zero)))
            g5.append(jnp.where(has5, rows_of(low_first, idx5), jnp.where(far5, far_high, zero)))
        for q in range(TILES):
            u, m = q // 16, q % 16
            gain = jnp.where(kk == 15, lane_roll(r5[u], 15 - m), zero)
            FL[f, q] = FL[f, q] + jnp.where(kk == 0, lane_roll(r4[u], -m), gain)
        half_rate = 0.5 * rate

        def emit(q, x, total):
            X[f, q] = X[f, q] + (x + half_rate * total)

        laplace(lambda q: FL[f, q], level, g4, g5, emit)

    send_octants(0)
    part_fine(0)

    @pl.when(fld == 1)
    def _():
        mix_copy(0).start()

    part_coarse(0)

    @pl.when(fld == 1)
    def _():
        mix_copy(4).start()

    mask_coarse()

    @pl.when(fld == 0)
    def _():
        factors_fine(0)
        factors_coarse(0)

    wait_octants(0)
    def take_seed(f, _):
        add_octants(0, f, lambda q: seed_fine[f, :, q * LANES : (q + 1) * LANES])
        return 0

    lax.fori_loop(0, FIELDS, take_seed, 0)
    weights(0, 0, 0)
    weights(4, COARSE, 1)

    def start(f, _):
        begin(0, f, f // 4)
        return 0

    lax.fori_loop(0, FIELDS + 1, start, 0)

    def rest(s, _):
        part_fine(s)

        @pl.when(fld == 1)
        def _():
            mix_copy(s).start()

        return 0

    lax.fori_loop(1, 4, rest, 0)
    part_coarse(1)

    @pl.when(fld == 1)
    def _():
        mix_copy(5).start()

    @pl.when(fld == 0)
    def _():
        factors_fine(1)
        factors_coarse(1)

    def turn(t, _):
        late = jnp.where(t >= 5, 1, 0)
        s = late * (1 + (t - 5) // 4)
        f = jnp.where(t >= 5, lax.rem(t + 3, 4), t)
        level = f // 4
        finish(s, f, level)

        @pl.when(level == 1)
        def _():
            send_octants(1)
            mask_coarse()

        @pl.when((s == 1) & (level == 0))
        def _():
            @pl.when(f == 0)
            def _():
                wait_octants(1)

            add_octants(1, f, lambda q: X[f, q])

        @pl.when((f == 0) | (level == 1))
        def _():
            weights(level * 4 + s + 1, f, level)

        begin(s + 1, f, level)

        @pl.when((f == 3) & (s < 2) & (fld == 0))
        def _():
            factors_fine(s + 2)

        return 0

    lax.fori_loop(0, 13, turn, 0)

    def last(t, _):
        f = lax.rem(t + 4, 5)
        level = f // 4
        finish(3 - 2 * level, f, level)

        @pl.when(level == 0)
        def _():
            for q in range(TILES):
                out_fine[f, :, q * LANES : (q + 1) * LANES] = X[f, q]

        @pl.when(level == 1)
        def _():
            for q in range(TILES):
                for v in range(FIELDS):
                    out_coarse[v, :, q * LANES : (q + 1) * LANES] = X[COARSE, q, 2 * v : 2 * v + 2, :]

        return 0

    lax.fori_loop(0, 5, last, 0)

    for rslot in range(2):
        for d in range(1, LINKS):
            octant_copy(rslot, d).wait_send()
    for s in range(4):
        for f in range(5 if s < 2 else 4):
            for way in range(2):
                halo_copy(s * 5 + f, way).wait_send()

    @pl.when(fld == 0)
    def _():
        for slot in range(6):
            w_copy(slot).wait_send()

    @pl.when(fld == 1)
    def _():
        for slot in range(6):
            mix_copy(slot).wait_send()


def shards(*args):
    n = lax.axis_size("blk")
    seed_fine, seed_coarse = args[0], args[1]
    vmem = pl.BlockSpec(memory_space=pltpu.VMEM)
    smem = pl.BlockSpec(memory_space=pltpu.SMEM)
    tile = (ROWS, LANES)

    def buffer(*lead):
        return pltpu.VMEM((*lead, *tile), jnp.float32)

    def table(*lead):
        return pltpu.VMEM((*lead, *tile), jnp.int32)

    dma = pltpu.SemaphoreType.DMA
    return pl.pallas_call(
        functools.partial(kernel, n),
        out_shape=(
            jax.ShapeDtypeStruct(seed_fine.shape, jnp.float32),
            jax.ShapeDtypeStruct(seed_coarse.shape, jnp.float32),
        ),
        in_specs=[vmem] * 4 + [smem] * 7,
        out_specs=(vmem, vmem),
        scratch_shapes=[
            buffer(5, TILES), buffer(5, TILES),
            buffer(6, TILES), buffer(6, TILES), buffer(6, TILES), buffer(6, TILES), buffer(6, TILES),
            buffer(20, 2, 4), buffer(20, 2, 4),
            buffer(2, LINKS, 3), buffer(2, LINKS, 3),
            table(12), table(12), table(4),
            buffer(5), buffer(5), buffer(5), buffer(4), buffer(2), table(2),
            pltpu.SMEM((2 * LINKS,), jnp.int32),
            dma((20, 2)), dma((20, 2)), dma((6,)), dma((6,)), dma((6,)), dma((6,)), dma((2, LINKS)), dma((2, LINKS)),
        ],
        compiler_params=pltpu.CompilerParams(
            collective_id=0, has_side_effects=True, vmem_limit_bytes=40 * 1024 * 1024
        ),
    )(*args)


def solution(mesh):
    return jax.shard_map(
        shards,
        mesh=mesh,
        in_specs=(
            P("fld", "blk", None),
            P("fld", "blk", None),
            P(None, "fld", "blk", None),
            P(None, "fld", "blk", None),
            P("fld"),
            P("fld"),
            P("blk", None),
            P("blk", None),
            P("blk", None),
            P("blk"),
            P("blk"),
        ),
        out_specs=(P("fld", "blk", None), P("fld", "blk", None)),
        check_vma=False,
    )
```

```python
import functools

import jax
import jax.numpy as jnp
from jax import lax
from jax.experimental import pallas as pl
from jax.experimental.pallas import tpu as pltpu
from jax.sharding import PartitionSpec as P

NSUB = 4
FIELDS = 4
ROWS = 8
LANES = 128
TILES = 32
LINKS = 8
COARSE = FIELDS
HEAT = 0.5
ENERGY = 2.0


def rows_of(x, idx):
    return jnp.take_along_axis(x, idx, axis=0, mode="promise_in_bounds")


def lanes_of(x, idx):
    return jnp.take_along_axis(x, idx, axis=1, mode="promise_in_bounds")


def lane_roll(x, steps):
    steps = steps % LANES
    return x if steps == 0 else pltpu.roll(x, steps, 1)


def row_roll(x, steps):
    return pltpu.roll(x, steps % ROWS, 0)


def kernel(
    n,
    seed_fine_in, seed_coarse_in, saved_fine_in, saved_coarse_in, diffusion_in, shares_in, fine_nbr_in, coarse_nbr_in,
    children_in, fine_counts_in, coarse_counts_in,
    out_fine, out_coarse,
    seed_fine, seed_coarse, saved_fine, saved_coarse, diffusion, shares, fine_nbr, coarse_nbr, children,
    fine_counts, coarse_counts, in_sem,
    X, FL, FF, GG, PM, MR, W, HS, HR, RS, RR, NI, NL, NR, RT, SH, FM, KM, HN, CN, OC,
    h_send, h_recv, w_send, w_recv, m_send, m_recv, r_send, r_recv,
):
    me = lax.axis_index("blk")
    fld = lax.axis_index("fld")
    partner = {"fld": 1 - fld}

    def at(d):
        return {"blk": lax.rem(me + (d + n), n)}

    barrier = pltpu.get_barrier_semaphore()
    pl.semaphore_signal(barrier, inc=1, device_id=partner, device_id_type=pl.DeviceIdType.MESH)
    for d in range(1, LINKS):
        for way in (d, -d):
            pl.semaphore_signal(barrier, inc=1, device_id=at(way), device_id_type=pl.DeviceIdType.MESH)

    small = [
        pltpu.make_async_copy(source, target, in_sem.at[i])
        for i, (source, target) in enumerate((
            (children_in, children), (seed_coarse_in, seed_coarse), (diffusion_in, diffusion), (shares_in, shares),
            (fine_nbr_in, fine_nbr), (coarse_nbr_in, coarse_nbr), (fine_counts_in, fine_counts),
            (coarse_counts_in, coarse_counts), (saved_coarse_in, saved_coarse), (seed_fine_in, seed_fine),
        ))
    ]
    large = [
        pltpu.make_async_copy(saved_fine_in.at[3 - s], saved_fine.at[3 - s], in_sem.at[10 + s]) for s in range(4)
    ]
    for copy in (*small[:8], large[0], *small[8:], *large[1:]):
        copy.start()

    shape = (ROWS, LANES)
    row = lax.broadcasted_iota(jnp.int32, shape, 0)
    lane = lax.broadcasted_iota(jnp.int32, shape, 1)
    kk = lane & 15
    even = (row & 1) == 0
    zero = jnp.zeros(shape, jnp.float32)

    def cols(q):
        return pl.ds(pl.multiple_of(q * LANES, LANES), LANES)

    for copy in small[:8]:
        copy.wait()

    def spread_rows(values):
        out = jnp.full(shape, values[0])
        for r in range(1, ROWS):
            out = jnp.where(row == r, values[r], out)
        return out

    for f in range(FIELDS):
        RT[f] = jnp.full(shape, diffusion[f])
        SH[f] = jnp.full(shape, shares[f])
        FM[f] = jnp.full(shape, jnp.where((fld == 0) & (f == 0), 1.0, 0.0))
    RT[COARSE] = spread_rows([0.5 * diffusion[r // 2] for r in range(ROWS)])
    SH[COARSE] = spread_rows([shares[r // 2] for r in range(ROWS)])
    FM[COARSE] = jnp.where((row < 2) & (fld == 0), 1.0, 0.0)
    CN[0] = spread_rows([fine_counts[r] for r in range(ROWS)])
    CN[1] = spread_rows([coarse_counts[r % 2] for r in range(ROWS)])
    for level in range(2):
        HN[level] = 1.0 / CN[level].astype(jnp.float32)
        for face in range(6):
            if level == 0:
                raw = spread_rows([fine_nbr[r, face] for r in range(ROWS)])
                base, per, idx = me * 8, 8, raw & 7
            else:
                raw = spread_rows([coarse_nbr[r % 2, face] for r in range(ROWS)])
                base, per, idx = me * 2, 2, (row & 6) + (raw & 1)
            there = raw >= 0
            local = there & (raw >= base) & (raw < base + per)
            NI[level * 6 + face] = idx
            NL[level * 6 + face] = jnp.where(local, 1, 0)
            if face >= 4:
                NR[level * 2 + face - 4] = jnp.where(there & ~local, 1, 0)

    for d in range(LINKS):
        octant, slot = jnp.int32(0), jnp.int32(0)
        for p in range(2):
            for o in range(8):
                child = children[p, o]
                hit = (child >= 0) & ((((child >> 3) - me) & (n - 1)) == d)
                octant = jnp.where(hit, p * 8 + o, octant)
                slot = jnp.where(hit, child & 7, slot)
        OC[d] = octant
        OC[LINKS + d] = slot
    keep = [[jnp.where(children[p, o] < 0, 1.0, 0.0) for o in range(8)] for p in range(2)]
    for ab in range(4):
        halves = [jnp.where(kk < 8, keep[p][2 * ab], keep[p][2 * ab + 1]) for p in range(2)]
        KM[ab] = jnp.where(even, halves[0], halves[1])

    def load_coarse(q, _):
        for f in range(FIELDS):
            X[COARSE, q, 2 * f : 2 * f + 2, :] = seed_coarse[f, :, cols(q)]
        return 0

    lax.fori_loop(0, TILES, load_coarse, 0, unroll=4)

    pl.semaphore_wait(barrier, 2 * (LINKS - 1) + 1)

    def octant_copy(rslot, d):
        return pltpu.make_async_remote_copy(
            src_ref=RS.at[rslot, d], dst_ref=RR.at[rslot, d], send_sem=r_send.at[rslot, d],
            recv_sem=r_recv.at[rslot, d], device_id=at(d), device_id_type=pl.DeviceIdType.MESH,
        )

    def send_octants(rslot):
        for d in (7, 6, 5, 4, 3, 2, 1, 0):
            octant = OC[d]
            p, a, b, c = octant >> 3, (octant >> 2) & 1, (octant >> 1) & 1, octant & 1
            parts = []
            for i in range(8):
                v = X[COARSE, (a * 8 + i) * 2 + b]
                v = jnp.where(jnp.full(shape, c) == 1, lane_roll(v, -8), v)
                v = jnp.where(jnp.full(shape, p) == 1, row_roll(v, -1), v)
                parts.append(v)
            target = RR if d == 0 else RS
            for u in range(2):
                pair = []
                for g in range(2):
                    at_i = u * 4 + g * 2
                    pair.append(jnp.where(kk < 8, parts[at_i], lane_roll(parts[at_i + 1], 8)))
                target[rslot, d, u] = jnp.where(even, pair[0], row_roll(pair[1], 1))
            target[rslot, d, 2] = jnp.full(shape, OC[LINKS + d]).astype(jnp.float32)
            if d:
                octant_copy(rslot, d).start()

    def mask_coarse():
        def one(i, _):
            for b in range(2):
                X[COARSE, i * 2 + b] = X[COARSE, i * 2 + b] * KM[(i >> 3) * 2 + b]
            return 0

        lax.fori_loop(0, 16, one, 0, unroll=4)

    def wait_octants(rslot):
        for d in range(1, LINKS):
            octant_copy(rslot, d).wait_recv()

    spread_idx = [
        [((lane >> 5) + jh * 4) * 16 + h * 8 + ((lane & 15) >> 1) for jh in range(2)] for h in range(2)
    ]

    def add_octants(rslot, f, source):
        mine = [RR[rslot, d, 2] == row.astype(jnp.float32) for d in range(LINKS)]
        for u in range(2):
            for g in range(2):
                total = zero
                for d in range(LINKS):
                    line = jnp.broadcast_to(RR[rslot, d, u, pl.ds(f * 2 + g, 1), :], shape)
                    total = jnp.where(mine[d], line, total)
                total = 0.125 * total
                for h in range(2):
                    i = (u * 4 + g * 2 + h) * 2
                    for jh in range(2):
                        gain = lanes_of(total, spread_idx[h][jh])
                        for q in (i * 2 + jh, (i + 1) * 2 + jh):
                            X[f, q] = source(q) + gain

    def mix_copy(slot):
        return pltpu.make_async_remote_copy(
            src_ref=PM.at[slot], dst_ref=MR.at[slot], send_sem=m_send.at[slot], recv_sem=m_recv.at[slot],
            device_id=partner, device_id_type=pl.DeviceIdType.MESH,
        )

    def part_fine(s):
        def one(q, _):
            total = SH[0] * saved_fine[3 - s, 0, :, cols(q)]
            for f in range(1, FIELDS):
                total = total + SH[f] * saved_fine[3 - s, f, :, cols(q)]
            PM[s, q] = total
            return 0

        lax.fori_loop(0, TILES, one, 0, unroll=4)

    def coarse_rows(c, f, q):
        first = jnp.broadcast_to(saved_coarse[c, f, 0:1, cols(q)], shape)
        return jnp.where(even, first, jnp.broadcast_to(saved_coarse[c, f, 1:2, cols(q)], shape))

    def part_coarse(s):
        def one(q, _):
            total = SH[0] * coarse_rows(1 - s, 0, q)
            for f in range(1, FIELDS):
                total = total + SH[f] * coarse_rows(1 - s, f, q)
            PM[4 + s, q] = total
            return 0

        lax.fori_loop(0, TILES, one, 0, unroll=4)

    def factors(slot, level, temperature):
        mix_copy(slot).wait_recv()

        def one(q, _):
            count = CN[level]
            half = HN[level] * HEAT
            mix = PM[slot, q] + MR[slot, q]
            t = temperature(q)
            saved = []
            for k in range(NSUB):
                inverse = 1.0 / t
                e = half * jnp.exp(-ENERGY * inverse)
                saved.append((inverse, e))
                if k + 1 < NSUB:
                    t = jnp.where(k < count, t + mix * e, t)
            f, g = jnp.ones(shape, jnp.float32), zero
            for k in reversed(range(NSUB)):
                inverse, e = saved[k]
                live = k < count
                g = jnp.where(live, g + e * f, g)
                f = jnp.where(live, f + f * (ENERGY * mix * e * (inverse * inverse)), f)
            FF[slot, q] = f
            GG[slot, q] = g
            return 0

        lax.fori_loop(0, TILES, one, 0, unroll=4)

    def factors_fine(s):
        factors(s, 0, lambda q: saved_fine[3 - s, 0, :, cols(q)])

    def factors_coarse(s):
        factors(4 + s, 1, lambda q: coarse_rows(1 - s, 0, q))

    def w_copy(slot):
        return pltpu.make_async_remote_copy(
            src_ref=W.at[slot], dst_ref=W.at[slot], send_sem=w_send.at[slot], recv_sem=w_recv.at[slot],
            device_id=partner, device_id_type=pl.DeviceIdType.MESH,
        )

    def weights(slot, f, level):
        @pl.when(fld == 0)
        def _():
            source = jnp.where(jnp.full(shape, level) == 1, row & 1, row)

            def one(q, _):
                W[slot, q] = GG[slot, q] * rows_of(X[f, q], source)
                return 0

            lax.fori_loop(0, TILES, one, 0, unroll=8)
            w_copy(slot).start()

        @pl.when(fld == 1)
        def _():
            w_copy(slot).wait_recv()

    def halo_copy(slot, way):
        return pltpu.make_async_remote_copy(
            src_ref=HS.at[slot, way], dst_ref=HR.at[slot, way], send_sem=h_send.at[slot, way],
            recv_sem=h_recv.at[slot, way], device_id=at(1 if way == 0 else -1),
            device_id_type=pl.DeviceIdType.MESH,
        )

    def laplace(v, level, g4, g5, emit):
        idx = [NI[level * 6 + face] for face in range(4)]
        has = [NL[level * 6 + face] > 0 for face in range(4)]

        def ghost(x, face):
            return jnp.where(has[face], rows_of(x, idx[face]), zero)

        for i in range(16):
            pair = [v(2 * i), v(2 * i + 1)]
            up = [lane_roll(x, 16) for x in pair]
            down = [lane_roll(x, -16) for x in pair]
            j_less = [jnp.where(lane < 16, ghost(up[1], 2), up[0]), jnp.where(lane < 16, up[0], up[1])]
            j_more = [
                jnp.where(lane >= 112, down[1], down[0]),
                jnp.where(lane >= 112, ghost(down[0], 3), down[1]),
            ]
            for jh in range(2):
                q = 2 * i + jh
                u, m = q // 16, q % 16
                x = pair[jh]
                i_less = v(q - 2) if i > 0 else ghost(v(30 + jh), 0)
                i_more = v(q + 2) if i < 15 else ghost(v(jh), 1)
                k_less = jnp.where(kk == 0, lane_roll(g4[u], -m), lane_roll(x, 1))
                k_more = jnp.where(kk == 15, lane_roll(g5[u], 15 - m), lane_roll(x, -1))
                total = ((i_less + i_more) + (j_less[jh] + j_more[jh])) + ((k_less + k_more) - 6.0 * x)
                emit(q, x, total)

    def pack(v, k):
        packed = []
        for u in range(2):
            out = zero
            for m in range(16):
                out = jnp.where(kk == m, lane_roll(v(u * 16 + m), m - k), out)
            packed.append(out)
        return packed

    def begin(s, f, level):
        slot = s * 5 + f
        wslot = level * 4 + s
        rate = RT[f]
        share = SH[f]
        scaled = FM[f] > 0

        for q in range(TILES):
            X[f, q] = X[f, q] * jnp.where(scaled, FF[wslot, q], 1.0) + share * W[wslot, q]
        low = pack(lambda q: X[f, q], 0)
        high = pack(lambda q: X[f, q], 15)
        idx4, idx5 = NI[level * 6 + 4], NI[level * 6 + 5]
        has4, has5 = NL[level * 6 + 4] > 0, NL[level * 6 + 5] > 0
        g4 = [jnp.where(has4, rows_of(x, idx4), zero) for x in high]
        g5 = [jnp.where(has5, rows_of(x, idx5), zero) for x in low]

        def emit(q, x, total):
            FL[f, q] = rate * total

        laplace(lambda q: X[f, q], level, g4, g5, emit)
        low_first = pack(lambda q: FL[f, q], 0)
        high_first = pack(lambda q: FL[f, q], 15)
        for u in range(2):
            HS[slot, 0, u] = high[u]
            HS[slot, 0, 2 + u] = high_first[u]
            HS[slot, 1, u] = low[u]
            HS[slot, 1, 2 + u] = low_first[u]
        halo_copy(slot, 0).start()
        halo_copy(slot, 1).start()

    def finish(s, f, level):
        slot = s * 5 + f
        rate = RT[f]
        halo_copy(slot, 0).wait_recv()
        halo_copy(slot, 1).wait_recv()
        idx4, idx5 = NI[level * 6 + 4], NI[level * 6 + 5]
        has4, has5 = NL[level * 6 + 4] > 0, NL[level * 6 + 5] > 0
        far4, far5 = NR[level * 2] > 0, NR[level * 2 + 1] > 0
        r4, r5, g4, g5 = [], [], [], []
        for u in range(2):
            r4.append(jnp.where(far4, rate * rows_of(HR[slot, 0, u], idx4), zero))
            r5.append(jnp.where(far5, rate * rows_of(HR[slot, 1, u], idx5), zero))
        for u in range(2):
            low_first = HS[slot, 1, 2 + u] + r4[u]
            high_first = HS[slot, 0, 2 + u] + r5[u]
            far_low = rows_of(HR[slot, 0, 2 + u], idx4) + rate * HS[slot, 1, u]
            far_high = rows_of(HR[slot, 1, 2 + u], idx5) + rate * HS[slot, 0, u]
            g4.append(jnp.where(has4, rows_of(high_first, idx4), jnp.where(far4, far_low, zero)))
            g5.append(jnp.where(has5, rows_of(low_first, idx5), jnp.where(far5, far_high, zero)))
        for q in range(TILES):
            u, m = q // 16, q % 16
            gain = jnp.where(kk == 15, lane_roll(r5[u], 15 - m), zero)
            FL[f, q] = FL[f, q] + jnp.where(kk == 0, lane_roll(r4[u], -m), gain)
        half_rate = 0.5 * rate

        def emit(q, x, total):
            X[f, q] = X[f, q] + (x + half_rate * total)

        laplace(lambda q: FL[f, q], level, g4, g5, emit)

    send_octants(0)
    for copy in (*large, small[8]):
        copy.wait()

    def parts(s, _):
        part_fine(s)

        @pl.when(fld == 1)
        def _():
            mix_copy(s).start()

        return 0

    lax.fori_loop(0, 4, parts, 0)

    def parts_coarse(s, _):
        part_coarse(s)

        @pl.when(fld == 1)
        def _():
            mix_copy(4 + s).start()

        return 0

    lax.fori_loop(0, 2, parts_coarse, 0)
    mask_coarse()

    @pl.when(fld == 0)
    def _():
        def fine(s, _):
            factors_fine(s)
            return 0

        def coarse(s, _):
            factors_coarse(s)
            return 0

        lax.fori_loop(0, 4, fine, 0)
        lax.fori_loop(0, 2, coarse, 0)

    small[9].wait()
    wait_octants(0)

    def take_seed(f, _):
        add_octants(0, f, lambda q: seed_fine[f, :, q * LANES : (q + 1) * LANES])
        return 0

    lax.fori_loop(0, FIELDS, take_seed, 0)
    weights(0, 0, 0)
    weights(4, COARSE, 1)

    def start(f, _):
        begin(0, f, f // 4)
        return 0

    lax.fori_loop(0, FIELDS + 1, start, 0)

    def turn(t, _):
        late = jnp.where(t >= 5, 1, 0)
        s = late * (1 + (t - 5) // 4)
        f = jnp.where(t >= 5, lax.rem(t + 3, 4), t)
        level = f // 4
        finish(s, f, level)

        @pl.when(level == 1)
        def _():
            send_octants(1)
            mask_coarse()

        @pl.when((s == 1) & (level == 0))
        def _():
            @pl.when(f == 0)
            def _():
                wait_octants(1)

            add_octants(1, f, lambda q: X[f, q])

        @pl.when((f == 0) | (level == 1))
        def _():
            weights(level * 4 + s + 1, f, level)

        begin(s + 1, f, level)

        return 0

    lax.fori_loop(0, 13, turn, 0)

    def last(t, _):
        f = lax.rem(t + 4, 5)
        level = f // 4
        finish(3 - 2 * level, f, level)

        @pl.when(level == 0)
        def _():
            for q in range(TILES):
                out_fine[f, :, q * LANES : (q + 1) * LANES] = X[f, q]

        @pl.when(level == 1)
        def _():
            for q in range(TILES):
                for v in range(FIELDS):
                    out_coarse[v, :, q * LANES : (q + 1) * LANES] = X[COARSE, q, 2 * v : 2 * v + 2, :]

        return 0

    lax.fori_loop(0, 5, last, 0)

    for rslot in range(2):
        for d in range(1, LINKS):
            octant_copy(rslot, d).wait_send()
    for s in range(4):
        for f in range(5 if s < 2 else 4):
            for way in range(2):
                halo_copy(s * 5 + f, way).wait_send()

    @pl.when(fld == 0)
    def _():
        for slot in range(6):
            w_copy(slot).wait_send()

    @pl.when(fld == 1)
    def _():
        for slot in range(6):
            mix_copy(slot).wait_send()


def shards(*args):
    n = lax.axis_size("blk")
    seed_fine, seed_coarse = args[0], args[1]
    vmem = pl.BlockSpec(memory_space=pltpu.VMEM)
    hbm = pl.BlockSpec(memory_space=pltpu.HBM)
    tile = (ROWS, LANES)

    def buffer(*lead):
        return pltpu.VMEM((*lead, *tile), jnp.float32)

    def table(*lead):
        return pltpu.VMEM((*lead, *tile), jnp.int32)

    dma = pltpu.SemaphoreType.DMA
    return pl.pallas_call(
        functools.partial(kernel, n),
        out_shape=(
            pltpu.VMEM(seed_fine.shape, jnp.float32),
            pltpu.VMEM(seed_coarse.shape, jnp.float32),
        ),
        in_specs=[hbm] * 11,
        out_specs=(vmem, vmem),
        scratch_shapes=[
            *(pltpu.VMEM(x.shape, jnp.float32) for x in args[:4]),
            *(pltpu.SMEM(x.shape, x.dtype) for x in args[4:]),
            dma((14,)),
            buffer(5, TILES), buffer(5, TILES),
            buffer(6, TILES), buffer(6, TILES), buffer(6, TILES), buffer(6, TILES), buffer(6, TILES),
            buffer(20, 2, 4), buffer(20, 2, 4),
            buffer(2, LINKS, 3), buffer(2, LINKS, 3),
            table(12), table(12), table(4),
            buffer(5), buffer(5), buffer(5), buffer(4), buffer(2), table(2),
            pltpu.SMEM((2 * LINKS,), jnp.int32),
            dma((20, 2)), dma((20, 2)), dma((6,)), dma((6,)), dma((6,)), dma((6,)), dma((2, LINKS)), dma((2, LINKS)),
        ],
        compiler_params=pltpu.CompilerParams(
            collective_id=0, has_side_effects=True, vmem_limit_bytes=62_000_000
        ),
    )(*args)


def solution(mesh):
    return jax.shard_map(
        shards,
        mesh=mesh,
        in_specs=(
            P("fld", "blk", None),
            P("fld", "blk", None),
            P(None, "fld", "blk", None),
            P(None, "fld", "blk", None),
            P("fld"),
            P("fld"),
            P("blk", None),
            P("blk", None),
            P("blk", None),
            P("blk"),
            P("blk"),
        ),
        out_specs=(P("fld", "blk", None), P("fld", "blk", None)),
        check_vma=False,
    )
```

```python
import functools

import jax
import jax.numpy as jnp
from jax import lax
from jax.experimental import pallas as pl
from jax.experimental.pallas import tpu as pltpu
from jax.sharding import PartitionSpec as P

NSUB = 4
FIELDS = 4
ROWS = 8
LANES = 128
TILES = 32
LINKS = 8
COARSE = FIELDS
HEAT = 0.5
ENERGY = 2.0


def rows_of(x, idx):
    return jnp.take_along_axis(x, idx, axis=0, mode="promise_in_bounds")


def lanes_of(x, idx):
    return jnp.take_along_axis(x, idx, axis=1, mode="promise_in_bounds")


def lane_roll(x, steps):
    steps = steps % LANES
    return x if steps == 0 else pltpu.roll(x, steps, 1)


def row_roll(x, steps):
    return pltpu.roll(x, steps % ROWS, 0)


def kernel(
    n,
    seed_fine_in, seed_coarse_in, saved_fine_in, saved_coarse_in, diffusion_in, shares_in, fine_nbr_in, coarse_nbr_in,
    children_in, fine_counts_in, coarse_counts_in,
    out_fine, out_coarse,
    seed_fine, seed_coarse, saved_fine, saved_coarse, diffusion, shares, fine_nbr, coarse_nbr, children,
    fine_counts, coarse_counts, in_sem,
    MX, X, FL, FF, GG, PM, MR, W, HS, HR, RS, RR, NI, NL, NR, RT, SH, FM, KM, HN, CN, OC,
    h_send, h_recv, w_send, w_recv, m_send, m_recv, r_send, r_recv,
):
    me = lax.axis_index("blk")
    fld = lax.axis_index("fld")
    partner = {"fld": 1 - fld}

    def at(d):
        return {"blk": lax.rem(me + (d + n), n)}

    barrier = pltpu.get_barrier_semaphore()
    pl.semaphore_signal(barrier, inc=1, device_id=partner, device_id_type=pl.DeviceIdType.MESH)
    for d in range(1, LINKS):
        for way in (d, -d):
            pl.semaphore_signal(barrier, inc=1, device_id=at(way), device_id_type=pl.DeviceIdType.MESH)

    small = [
        pltpu.make_async_copy(source, target, in_sem.at[i])
        for i, (source, target) in enumerate((
            (children_in, children), (seed_coarse_in, seed_coarse), (diffusion_in, diffusion), (shares_in, shares),
            (fine_nbr_in, fine_nbr), (coarse_nbr_in, coarse_nbr), (fine_counts_in, fine_counts),
            (coarse_counts_in, coarse_counts), (saved_coarse_in, saved_coarse), (seed_fine_in, seed_fine),
        ))
    ]
    large = [
        pltpu.make_async_copy(saved_fine_in.at[3 - s], saved_fine.at[3 - s], in_sem.at[10 + s]) for s in range(4)
    ]
    for copy in (*small[:8], large[0], *small[8:], *large[1:]):
        copy.start()

    shape = (ROWS, LANES)
    row = lax.broadcasted_iota(jnp.int32, shape, 0)
    lane = lax.broadcasted_iota(jnp.int32, shape, 1)
    kk = lane & 15
    even = (row & 1) == 0
    zero = jnp.zeros(shape, jnp.float32)

    def cols(q):
        return pl.ds(pl.multiple_of(q * LANES, LANES), LANES)

    for copy in small[:8]:
        copy.wait()

    def spread_rows(values):
        out = jnp.full(shape, values[0])
        for r in range(1, ROWS):
            out = jnp.where(row == r, values[r], out)
        return out

    for f in range(FIELDS):
        RT[f] = jnp.full(shape, diffusion[f])
        SH[f] = jnp.full(shape, shares[f])
        FM[f] = jnp.full(shape, jnp.where((fld == 0) & (f == 0), 1.0, 0.0))
    RT[COARSE] = spread_rows([0.5 * diffusion[r // 2] for r in range(ROWS)])
    SH[COARSE] = spread_rows([shares[r // 2] for r in range(ROWS)])
    FM[COARSE] = jnp.where((row < 2) & (fld == 0), 1.0, 0.0)
    CN[0] = spread_rows([fine_counts[r] for r in range(ROWS)])
    CN[1] = spread_rows([coarse_counts[r % 2] for r in range(ROWS)])
    for level in range(2):
        HN[level] = 1.0 / CN[level].astype(jnp.float32)
        for face in range(6):
            if level == 0:
                raw = spread_rows([fine_nbr[r, face] for r in range(ROWS)])
                base, per, idx = me * 8, 8, raw & 7
            else:
                raw = spread_rows([coarse_nbr[r % 2, face] for r in range(ROWS)])
                base, per, idx = me * 2, 2, (row & 6) + (raw & 1)
            there = raw >= 0
            local = there & (raw >= base) & (raw < base + per)
            NI[level * 6 + face] = idx
            NL[level * 6 + face] = jnp.where(local, 1, 0)
            if face >= 4:
                NR[level * 2 + face - 4] = jnp.where(there & ~local, 1, 0)

    for d in range(LINKS):
        octant, slot = jnp.int32(0), jnp.int32(0)
        for p in range(2):
            for o in range(8):
                child = children[p, o]
                hit = (child >= 0) & ((((child >> 3) - me) & (n - 1)) == d)
                octant = jnp.where(hit, p * 8 + o, octant)
                slot = jnp.where(hit, child & 7, slot)
        OC[d] = octant
        OC[LINKS + d] = slot
    keep = [[jnp.where(children[p, o] < 0, 1.0, 0.0) for o in range(8)] for p in range(2)]
    for ab in range(4):
        halves = [jnp.where(kk < 8, keep[p][2 * ab], keep[p][2 * ab + 1]) for p in range(2)]
        KM[ab] = jnp.where(even, halves[0], halves[1])

    def load_coarse(q, _):
        for f in range(FIELDS):
            X[COARSE, q, 2 * f : 2 * f + 2, :] = seed_coarse[f, :, cols(q)]
        return 0

    lax.fori_loop(0, TILES, load_coarse, 0, unroll=4)

    pl.semaphore_wait(barrier, 2 * (LINKS - 1) + 1)

    def octant_copy(rslot, d):
        return pltpu.make_async_remote_copy(
            src_ref=RS.at[rslot, d], dst_ref=RR.at[rslot, d], send_sem=r_send.at[rslot, d],
            recv_sem=r_recv.at[rslot, d], device_id=at(d), device_id_type=pl.DeviceIdType.MESH,
        )

    def send_octants(rslot):
        for d in (7, 6, 5, 4, 3, 2, 1, 0):
            octant = OC[d]
            p, a, b, c = octant >> 3, (octant >> 2) & 1, (octant >> 1) & 1, octant & 1
            parts = []
            for i in range(8):
                v = X[COARSE, (a * 8 + i) * 2 + b]
                v = jnp.where(jnp.full(shape, c) == 1, lane_roll(v, -8), v)
                v = jnp.where(jnp.full(shape, p) == 1, row_roll(v, -1), v)
                parts.append(v)
            target = RR if d == 0 else RS
            for u in range(2):
                pair = []
                for g in range(2):
                    at_i = u * 4 + g * 2
                    pair.append(jnp.where(kk < 8, parts[at_i], lane_roll(parts[at_i + 1], 8)))
                target[rslot, d, u] = jnp.where(even, pair[0], row_roll(pair[1], 1))
            target[rslot, d, 2] = jnp.full(shape, OC[LINKS + d]).astype(jnp.float32)
            if d:
                octant_copy(rslot, d).start()

    def mask_coarse():
        def one(i, _):
            for b in range(2):
                X[COARSE, i * 2 + b] = X[COARSE, i * 2 + b] * KM[(i >> 3) * 2 + b]
            return 0

        lax.fori_loop(0, 16, one, 0, unroll=4)

    def wait_octants(rslot):
        for d in range(1, LINKS):
            octant_copy(rslot, d).wait_recv()

    spread_idx = [
        [((lane >> 5) + jh * 4) * 16 + h * 8 + ((lane & 15) >> 1) for jh in range(2)] for h in range(2)
    ]

    def add_octants(rslot, f, source):
        mine = [RR[rslot, d, 2] == row.astype(jnp.float32) for d in range(LINKS)]
        for u in range(2):
            for g in range(2):
                total = zero
                for d in range(LINKS):
                    line = jnp.broadcast_to(RR[rslot, d, u, pl.ds(f * 2 + g, 1), :], shape)
                    total = jnp.where(mine[d], line, total)
                total = 0.125 * total
                for h in range(2):
                    i = (u * 4 + g * 2 + h) * 2
                    for jh in range(2):
                        gain = lanes_of(total, spread_idx[h][jh])
                        for q in (i * 2 + jh, (i + 1) * 2 + jh):
                            X[f, q] = source(q) + gain

    def mix_copy(slot):
        return pltpu.make_async_remote_copy(
            src_ref=PM.at[slot], dst_ref=MR.at[slot], send_sem=m_send.at[slot], recv_sem=m_recv.at[slot],
            device_id=partner, device_id_type=pl.DeviceIdType.MESH,
        )

    def part_fine(s):
        def one(q, _):
            total = SH[0] * saved_fine[3 - s, 0, :, cols(q)]
            for f in range(1, FIELDS):
                total = total + SH[f] * saved_fine[3 - s, f, :, cols(q)]
            PM[s, q] = total
            return 0

        lax.fori_loop(0, TILES, one, 0, unroll=4)

    def coarse_rows(c, f, q):
        first = jnp.broadcast_to(saved_coarse[c, f, 0:1, cols(q)], shape)
        return jnp.where(even, first, jnp.broadcast_to(saved_coarse[c, f, 1:2, cols(q)], shape))

    def part_coarse(s):
        def one(q, _):
            total = SH[0] * coarse_rows(1 - s, 0, q)
            for f in range(1, FIELDS):
                total = total + SH[f] * coarse_rows(1 - s, f, q)
            PM[4 + s, q] = total
            return 0

        lax.fori_loop(0, TILES, one, 0, unroll=4)

    def factors(slot, level, temperature):
        mix_copy(slot).wait_recv()

        def one(q, _):
            count = CN[level]
            half = HN[level] * HEAT
            mix = PM[slot, q] + MR[slot, q]
            t = temperature(q)
            saved = []
            for k in range(NSUB):
                inverse = 1.0 / t
                e = half * jnp.exp(-ENERGY * inverse)
                saved.append((inverse, e))
                if k + 1 < NSUB:
                    t = jnp.where(k < count, t + mix * e, t)
            f, g = jnp.ones(shape, jnp.float32), zero
            for k in reversed(range(NSUB)):
                inverse, e = saved[k]
                live = k < count
                g = jnp.where(live, g + e * f, g)
                f = jnp.where(live, f + f * (ENERGY * mix * e * (inverse * inverse)), f)
            FF[slot, q] = f
            GG[slot, q] = g
            return 0

        lax.fori_loop(0, TILES, one, 0, unroll=4)

    def factors_fine(s):
        factors(s, 0, lambda q: saved_fine[3 - s, 0, :, cols(q)])

    def factors_coarse(s):
        factors(4 + s, 1, lambda q: coarse_rows(1 - s, 0, q))

    def w_copy(slot):
        return pltpu.make_async_remote_copy(
            src_ref=W.at[slot], dst_ref=W.at[slot], send_sem=w_send.at[slot], recv_sem=w_recv.at[slot],
            device_id=partner, device_id_type=pl.DeviceIdType.MESH,
        )

    def weights(slot, f, level):
        @pl.when(fld == 0)
        def _():
            source = jnp.where(jnp.full(shape, level) == 1, row & 1, row)

            def one(q, _):
                W[slot, q] = GG[slot, q] * rows_of(X[f, q], source)
                return 0

            lax.fori_loop(0, TILES, one, 0, unroll=8)
            w_copy(slot).start()

        @pl.when(fld == 1)
        def _():
            w_copy(slot).wait_recv()

    def halo_copy(slot, way):
        return pltpu.make_async_remote_copy(
            src_ref=HS.at[slot, way], dst_ref=HR.at[slot, way], send_sem=h_send.at[slot, way],
            recv_sem=h_recv.at[slot, way], device_id=at(1 if way == 0 else -1),
            device_id_type=pl.DeviceIdType.MESH,
        )

    def stencil_matrix():
        def one(r, _):
            source = r * ROWS * 2 + lax.broadcasted_iota(jnp.int32, (2 * ROWS, 2 * LANES), 0)
            target = lax.broadcasted_iota(jnp.int32, (2 * ROWS, 2 * LANES), 1)
            apart = jnp.abs(source - target)
            near = (apart == 16) | ((apart == 1) & ((source >> 4) == (target >> 4)))
            entry = jnp.where(near, 1.0, jnp.where(apart == 0, -6.0, 0.0))
            MX[pl.ds(pl.multiple_of(r * ROWS * 2, ROWS * 2), ROWS * 2), :] = entry.astype(jnp.bfloat16)
            return 0

        lax.fori_loop(0, 16, one, 0)

    def laplace(v, level, g4, g5, emit):
        idx = [NI[level * 6 + face] for face in range(4)]
        has = [NL[level * 6 + face] > 0 for face in range(4)]

        def ghost(x, face):
            return jnp.where(has[face], rows_of(x, idx[face]), zero)

        matrix = MX[...]
        planes = jnp.concatenate(
            [jnp.concatenate([v(2 * i + jh) for i in range(16)], axis=0) for jh in range(2)], axis=1
        )
        inner = None
        for piece in range(3):
            rounded = planes.astype(jnp.bfloat16)
            term = jnp.dot(rounded, matrix, preferred_element_type=jnp.float32)
            inner = term if inner is None else inner + term
            if piece < 2:
                planes = planes - rounded.astype(jnp.float32)

        for i in range(16):
            j_edge = [
                jnp.where(lane < 16, ghost(lane_roll(v(2 * i + 1), 16), 2), zero),
                jnp.where(lane >= 112, ghost(lane_roll(v(2 * i), -16), 3), zero),
            ]
            for jh in range(2):
                q = 2 * i + jh
                u, m = q // 16, q % 16
                i_less = v(q - 2) if i > 0 else ghost(v(30 + jh), 0)
                i_more = v(q + 2) if i < 15 else ghost(v(jh), 1)
                k_edge = jnp.where(kk == 15, lane_roll(g5[u], 15 - m), zero)
                k_edge = jnp.where(kk == 0, lane_roll(g4[u], -m), k_edge)
                plane = inner[i * ROWS : (i + 1) * ROWS, jh * LANES : (jh + 1) * LANES]
                emit(q, v(q), ((i_less + i_more) + (j_edge[jh] + k_edge)) + plane)

    def pack(v, k):
        packed = []
        for u in range(2):
            out = zero
            for m in range(16):
                out = jnp.where(kk == m, lane_roll(v(u * 16 + m), m - k), out)
            packed.append(out)
        return packed

    def begin(s, f, level):
        slot = s * 5 + f
        wslot = level * 4 + s
        rate = RT[f]
        share = SH[f]
        scaled = FM[f] > 0

        for q in range(TILES):
            X[f, q] = X[f, q] * jnp.where(scaled, FF[wslot, q], 1.0) + share * W[wslot, q]
        low = pack(lambda q: X[f, q], 0)
        high = pack(lambda q: X[f, q], 15)
        idx4, idx5 = NI[level * 6 + 4], NI[level * 6 + 5]
        has4, has5 = NL[level * 6 + 4] > 0, NL[level * 6 + 5] > 0
        g4 = [jnp.where(has4, rows_of(x, idx4), zero) for x in high]
        g5 = [jnp.where(has5, rows_of(x, idx5), zero) for x in low]

        def emit(q, x, total):
            FL[f, q] = rate * total

        laplace(lambda q: X[f, q], level, g4, g5, emit)
        low_first = pack(lambda q: FL[f, q], 0)
        high_first = pack(lambda q: FL[f, q], 15)
        for u in range(2):
            HS[slot, 0, u] = high[u]
            HS[slot, 0, 2 + u] = high_first[u]
            HS[slot, 1, u] = low[u]
            HS[slot, 1, 2 + u] = low_first[u]
        halo_copy(slot, 0).start()
        halo_copy(slot, 1).start()

    def finish(s, f, level):
        slot = s * 5 + f
        rate = RT[f]
        halo_copy(slot, 0).wait_recv()
        halo_copy(slot, 1).wait_recv()
        idx4, idx5 = NI[level * 6 + 4], NI[level * 6 + 5]
        has4, has5 = NL[level * 6 + 4] > 0, NL[level * 6 + 5] > 0
        far4, far5 = NR[level * 2] > 0, NR[level * 2 + 1] > 0
        r4, r5, g4, g5 = [], [], [], []
        for u in range(2):
            r4.append(jnp.where(far4, rate * rows_of(HR[slot, 0, u], idx4), zero))
            r5.append(jnp.where(far5, rate * rows_of(HR[slot, 1, u], idx5), zero))
        for u in range(2):
            low_first = HS[slot, 1, 2 + u] + r4[u]
            high_first = HS[slot, 0, 2 + u] + r5[u]
            far_low = rows_of(HR[slot, 0, 2 + u], idx4) + rate * HS[slot, 1, u]
            far_high = rows_of(HR[slot, 1, 2 + u], idx5) + rate * HS[slot, 0, u]
            g4.append(jnp.where(has4, rows_of(high_first, idx4), jnp.where(far4, far_low, zero)))
            g5.append(jnp.where(has5, rows_of(low_first, idx5), jnp.where(far5, far_high, zero)))
        for q in range(TILES):
            u, m = q // 16, q % 16
            gain = jnp.where(kk == 15, lane_roll(r5[u], 15 - m), zero)
            FL[f, q] = FL[f, q] + jnp.where(kk == 0, lane_roll(r4[u], -m), gain)
        half_rate = 0.5 * rate

        def emit(q, x, total):
            X[f, q] = X[f, q] + (x + half_rate * total)

        laplace(lambda q: FL[f, q], level, g4, g5, emit)

    send_octants(0)
    stencil_matrix()
    for copy in (*large, small[8]):
        copy.wait()

    def parts(s, _):
        part_fine(s)

        @pl.when(fld == 1)
        def _():
            mix_copy(s).start()

        return 0

    lax.fori_loop(0, 4, parts, 0)

    def parts_coarse(s, _):
        part_coarse(s)

        @pl.when(fld == 1)
        def _():
            mix_copy(4 + s).start()

        return 0

    lax.fori_loop(0, 2, parts_coarse, 0)
    mask_coarse()

    @pl.when(fld == 0)
    def _():
        def fine(s, _):
            factors_fine(s)
            return 0

        def coarse(s, _):
            factors_coarse(s)
            return 0

        lax.fori_loop(0, 4, fine, 0)
        lax.fori_loop(0, 2, coarse, 0)

    small[9].wait()
    wait_octants(0)

    def take_seed(f, _):
        add_octants(0, f, lambda q: seed_fine[f, :, q * LANES : (q + 1) * LANES])
        return 0

    lax.fori_loop(0, FIELDS, take_seed, 0)
    weights(0, 0, 0)
    weights(4, COARSE, 1)

    def start(f, _):
        begin(0, f, f // 4)
        return 0

    lax.fori_loop(0, FIELDS + 1, start, 0)

    def turn(t, _):
        late = jnp.where(t >= 5, 1, 0)
        s = late * (1 + (t - 5) // 4)
        f = jnp.where(t >= 5, lax.rem(t + 3, 4), t)
        level = f // 4
        finish(s, f, level)

        @pl.when(level == 1)
        def _():
            send_octants(1)
            mask_coarse()

        @pl.when((s == 1) & (level == 0))
        def _():
            @pl.when(f == 0)
            def _():
                wait_octants(1)

            add_octants(1, f, lambda q: X[f, q])

        @pl.when((f == 0) | (level == 1))
        def _():
            weights(level * 4 + s + 1, f, level)

        begin(s + 1, f, level)

        return 0

    lax.fori_loop(0, 13, turn, 0)

    def last(t, _):
        f = lax.rem(t + 4, 5)
        level = f // 4
        finish(3 - 2 * level, f, level)

        @pl.when(level == 0)
        def _():
            for q in range(TILES):
                out_fine[f, :, q * LANES : (q + 1) * LANES] = X[f, q]

        @pl.when(level == 1)
        def _():
            for q in range(TILES):
                for v in range(FIELDS):
                    out_coarse[v, :, q * LANES : (q + 1) * LANES] = X[COARSE, q, 2 * v : 2 * v + 2, :]

        return 0

    lax.fori_loop(0, 5, last, 0)

    for rslot in range(2):
        for d in range(1, LINKS):
            octant_copy(rslot, d).wait_send()
    for s in range(4):
        for f in range(5 if s < 2 else 4):
            for way in range(2):
                halo_copy(s * 5 + f, way).wait_send()

    @pl.when(fld == 0)
    def _():
        for slot in range(6):
            w_copy(slot).wait_send()

    @pl.when(fld == 1)
    def _():
        for slot in range(6):
            mix_copy(slot).wait_send()


def shards(*args):
    n = lax.axis_size("blk")
    seed_fine, seed_coarse = args[0], args[1]
    vmem = pl.BlockSpec(memory_space=pltpu.VMEM)
    hbm = pl.BlockSpec(memory_space=pltpu.HBM)
    tile = (ROWS, LANES)

    def buffer(*lead):
        return pltpu.VMEM((*lead, *tile), jnp.float32)

    def table(*lead):
        return pltpu.VMEM((*lead, *tile), jnp.int32)

    dma = pltpu.SemaphoreType.DMA
    return pl.pallas_call(
        functools.partial(kernel, n),
        out_shape=(
            pltpu.VMEM(seed_fine.shape, jnp.float32),
            pltpu.VMEM(seed_coarse.shape, jnp.float32),
        ),
        in_specs=[hbm] * 11,
        out_specs=(vmem, vmem),
        scratch_shapes=[
            *(pltpu.VMEM(x.shape, jnp.float32) for x in args[:4]),
            *(pltpu.SMEM(x.shape, x.dtype) for x in args[4:]),
            dma((14,)),
            pltpu.VMEM((2 * LANES, 2 * LANES), jnp.bfloat16),
            buffer(5, TILES), buffer(5, TILES),
            buffer(6, TILES), buffer(6, TILES), buffer(6, TILES), buffer(6, TILES), buffer(6, TILES),
            buffer(20, 2, 4), buffer(20, 2, 4),
            buffer(2, LINKS, 3), buffer(2, LINKS, 3),
            table(12), table(12), table(4),
            buffer(5), buffer(5), buffer(5), buffer(4), buffer(2), table(2),
            pltpu.SMEM((2 * LINKS,), jnp.int32),
            dma((20, 2)), dma((20, 2)), dma((6,)), dma((6,)), dma((6,)), dma((6,)), dma((2, LINKS)), dma((2, LINKS)),
        ],
        compiler_params=pltpu.CompilerParams(
            collective_id=0, has_side_effects=True, vmem_limit_bytes=62_000_000
        ),
    )(*args)


def solution(mesh):
    return jax.shard_map(
        shards,
        mesh=mesh,
        in_specs=(
            P("fld", "blk", None),
            P("fld", "blk", None),
            P(None, "fld", "blk", None),
            P(None, "fld", "blk", None),
            P("fld"),
            P("fld"),
            P("blk", None),
            P("blk", None),
            P("blk", None),
            P("blk"),
            P("blk"),
        ),
        out_specs=(P("fld", "blk", None), P("fld", "blk", None)),
        check_vma=False,
    )
```

```python
import functools

import jax
import jax.numpy as jnp
from jax import lax
from jax.experimental import pallas as pl
from jax.experimental.pallas import tpu as pltpu
from jax.sharding import PartitionSpec as P

NSUB = 4
FIELDS = 4
ROWS = 8
LANES = 128
TILES = 32
LINKS = 8
COARSE = FIELDS
HEAT = 0.5
ENERGY = 2.0


def rows_of(x, idx):
    return jnp.take_along_axis(x, idx, axis=0, mode="promise_in_bounds")


def lanes_of(x, idx):
    return jnp.take_along_axis(x, idx, axis=1, mode="promise_in_bounds")


def lane_roll(x, steps):
    steps = steps % LANES
    return x if steps == 0 else pltpu.roll(x, steps, 1)


def row_roll(x, steps):
    return pltpu.roll(x, steps % ROWS, 0)


def kernel(
    n,
    seed_fine_in, seed_coarse_in, saved_fine_in, saved_coarse_in, diffusion_in, shares_in, fine_nbr_in, coarse_nbr_in,
    children_in, fine_counts_in, coarse_counts_in,
    out_fine, out_coarse,
    seed_fine, seed_coarse, saved_fine, saved_coarse, diffusion, shares, fine_nbr, coarse_nbr, children,
    fine_counts, coarse_counts, in_sem,
    MX, X, FL, FF, GG, PM, MR, W, HS, HR, RS, RR, NI, NL, NR, RT, SH, FM, KM, HN, CN, OC,
    h_send, h_recv, w_send, w_recv, m_send, m_recv, r_send, r_recv,
):
    me = lax.axis_index("blk")
    fld = lax.axis_index("fld")
    partner = {"fld": 1 - fld}

    def at(d):
        return {"blk": lax.rem(me + (d + n), n)}

    barrier = pltpu.get_barrier_semaphore()
    pl.semaphore_signal(barrier, inc=1, device_id=partner, device_id_type=pl.DeviceIdType.MESH)
    for d in range(1, LINKS):
        for way in (d, -d):
            pl.semaphore_signal(barrier, inc=1, device_id=at(way), device_id_type=pl.DeviceIdType.MESH)

    small = [
        pltpu.make_async_copy(source, target, in_sem.at[i])
        for i, (source, target) in enumerate((
            (children_in, children), (seed_coarse_in, seed_coarse), (diffusion_in, diffusion), (shares_in, shares),
            (fine_nbr_in, fine_nbr), (coarse_nbr_in, coarse_nbr), (fine_counts_in, fine_counts),
            (coarse_counts_in, coarse_counts), (saved_coarse_in, saved_coarse), (seed_fine_in, seed_fine),
        ))
    ]
    large = [
        pltpu.make_async_copy(saved_fine_in.at[3 - s], saved_fine.at[3 - s], in_sem.at[10 + s]) for s in range(4)
    ]
    for copy in (*small[:8], large[0], *small[8:], *large[1:]):
        copy.start()

    shape = (ROWS, LANES)
    row = lax.broadcasted_iota(jnp.int32, shape, 0)
    lane = lax.broadcasted_iota(jnp.int32, shape, 1)
    kk = lane & 15
    even = (row & 1) == 0
    zero = jnp.zeros(shape, jnp.float32)

    def cols(q):
        return pl.ds(pl.multiple_of(q * LANES, LANES), LANES)

    for copy in small[:8]:
        copy.wait()

    def spread_rows(values):
        out = jnp.full(shape, values[0])
        for r in range(1, ROWS):
            out = jnp.where(row == r, values[r], out)
        return out

    for f in range(FIELDS):
        RT[f] = jnp.full(shape, diffusion[f])
        SH[f] = jnp.full(shape, shares[f])
        FM[f] = jnp.full(shape, jnp.where((fld == 0) & (f == 0), 1.0, 0.0))
    RT[COARSE] = spread_rows([0.5 * diffusion[r // 2] for r in range(ROWS)])
    SH[COARSE] = spread_rows([shares[r // 2] for r in range(ROWS)])
    FM[COARSE] = jnp.where((row < 2) & (fld == 0), 1.0, 0.0)
    CN[0] = spread_rows([fine_counts[r] for r in range(ROWS)])
    CN[1] = spread_rows([coarse_counts[r % 2] for r in range(ROWS)])
    for level in range(2):
        HN[level] = 1.0 / CN[level].astype(jnp.float32)
        for face in range(6):
            if level == 0:
                raw = spread_rows([fine_nbr[r, face] for r in range(ROWS)])
                base, per, idx = me * 8, 8, raw & 7
            else:
                raw = spread_rows([coarse_nbr[r % 2, face] for r in range(ROWS)])
                base, per, idx = me * 2, 2, (row & 6) + (raw & 1)
            there = raw >= 0
            local = there & (raw >= base) & (raw < base + per)
            NI[level * 6 + face] = idx
            NL[level * 6 + face] = jnp.where(local, 1, 0)
            if face >= 4:
                NR[level * 2 + face - 4] = jnp.where(there & ~local, 1, 0)

    for d in range(LINKS):
        octant, slot = jnp.int32(0), jnp.int32(0)
        for p in range(2):
            for o in range(8):
                child = children[p, o]
                hit = (child >= 0) & ((((child >> 3) - me) & (n - 1)) == d)
                octant = jnp.where(hit, p * 8 + o, octant)
                slot = jnp.where(hit, child & 7, slot)
        OC[d] = octant
        OC[LINKS + d] = slot
    keep = [[jnp.where(children[p, o] < 0, 1.0, 0.0) for o in range(8)] for p in range(2)]
    for ab in range(4):
        halves = [jnp.where(kk < 8, keep[p][2 * ab], keep[p][2 * ab + 1]) for p in range(2)]
        KM[ab] = jnp.where(even, halves[0], halves[1])

    def load_coarse(q, _):
        for f in range(FIELDS):
            X[COARSE, q, 2 * f : 2 * f + 2, :] = seed_coarse[f, :, cols(q)]
        return 0

    lax.fori_loop(0, TILES, load_coarse, 0, unroll=4)

    pl.semaphore_wait(barrier, 2 * (LINKS - 1) + 1)

    def octant_copy(rslot, d):
        return pltpu.make_async_remote_copy(
            src_ref=RS.at[rslot, d], dst_ref=RR.at[rslot, d], send_sem=r_send.at[rslot, d],
            recv_sem=r_recv.at[rslot, d], device_id=at(d), device_id_type=pl.DeviceIdType.MESH,
        )

    def send_octants(rslot):
        for d in (7, 6, 5, 4, 3, 2, 1, 0):
            octant = OC[d]
            p, a, b, c = octant >> 3, (octant >> 2) & 1, (octant >> 1) & 1, octant & 1
            parts = []
            for i in range(8):
                v = X[COARSE, (a * 8 + i) * 2 + b]
                v = jnp.where(jnp.full(shape, c) == 1, lane_roll(v, -8), v)
                v = jnp.where(jnp.full(shape, p) == 1, row_roll(v, -1), v)
                parts.append(v)
            target = RR if d == 0 else RS
            for u in range(2):
                pair = []
                for g in range(2):
                    at_i = u * 4 + g * 2
                    pair.append(jnp.where(kk < 8, parts[at_i], lane_roll(parts[at_i + 1], 8)))
                target[rslot, d, u] = jnp.where(even, pair[0], row_roll(pair[1], 1))
            target[rslot, d, 2] = jnp.full(shape, OC[LINKS + d]).astype(jnp.float32)
            if d:
                octant_copy(rslot, d).start()

    def mask_coarse():
        def one(i, _):
            for b in range(2):
                X[COARSE, i * 2 + b] = X[COARSE, i * 2 + b] * KM[(i >> 3) * 2 + b]
            return 0

        lax.fori_loop(0, 16, one, 0, unroll=4)

    def wait_octants(rslot):
        for d in range(1, LINKS):
            octant_copy(rslot, d).wait_recv()

    spread_idx = [
        [((lane >> 5) + jh * 4) * 16 + h * 8 + ((lane & 15) >> 1) for jh in range(2)] for h in range(2)
    ]

    def add_octants(rslot, f, source):
        mine = [RR[rslot, d, 2] == row.astype(jnp.float32) for d in range(LINKS)]
        for u in range(2):
            for g in range(2):
                total = zero
                for d in range(LINKS):
                    line = jnp.broadcast_to(RR[rslot, d, u, pl.ds(f * 2 + g, 1), :], shape)
                    total = jnp.where(mine[d], line, total)
                total = 0.125 * total
                for h in range(2):
                    i = (u * 4 + g * 2 + h) * 2
                    for jh in range(2):
                        gain = lanes_of(total, spread_idx[h][jh])
                        for q in (i * 2 + jh, (i + 1) * 2 + jh):
                            X[f, q] = source(q) + gain

    def mix_copy(slot):
        return pltpu.make_async_remote_copy(
            src_ref=PM.at[slot], dst_ref=MR.at[slot], send_sem=m_send.at[slot], recv_sem=m_recv.at[slot],
            device_id=partner, device_id_type=pl.DeviceIdType.MESH,
        )

    def part_fine(s):
        def one(q, _):
            total = SH[0] * saved_fine[3 - s, 0, :, cols(q)]
            for f in range(1, FIELDS):
                total = total + SH[f] * saved_fine[3 - s, f, :, cols(q)]
            PM[s, q] = total
            return 0

        lax.fori_loop(0, TILES, one, 0, unroll=4)

    def coarse_rows(c, f, q):
        first = jnp.broadcast_to(saved_coarse[c, f, 0:1, cols(q)], shape)
        return jnp.where(even, first, jnp.broadcast_to(saved_coarse[c, f, 1:2, cols(q)], shape))

    def part_coarse(s):
        def one(q, _):
            total = SH[0] * coarse_rows(1 - s, 0, q)
            for f in range(1, FIELDS):
                total = total + SH[f] * coarse_rows(1 - s, f, q)
            PM[4 + s, q] = total
            return 0

        lax.fori_loop(0, TILES, one, 0, unroll=4)

    def factors(slot, level, temperature):
        mix_copy(slot).wait_recv()

        def one(q, _):
            count = CN[level]
            half = HN[level] * HEAT
            mix = PM[slot, q] + MR[slot, q]
            t = temperature(q)
            saved = []
            for k in range(NSUB):
                inverse = 1.0 / t
                e = half * jnp.exp(-ENERGY * inverse)
                saved.append((inverse, e))
                if k + 1 < NSUB:
                    t = jnp.where(k < count, t + mix * e, t)
            f, g = jnp.ones(shape, jnp.float32), zero
            for k in reversed(range(NSUB)):
                inverse, e = saved[k]
                live = k < count
                g = jnp.where(live, g + e * f, g)
                f = jnp.where(live, f + f * (ENERGY * mix * e * (inverse * inverse)), f)
            FF[slot, q] = f
            GG[slot, q] = g
            return 0

        lax.fori_loop(0, TILES, one, 0, unroll=4)

    def factors_fine(s):
        factors(s, 0, lambda q: saved_fine[3 - s, 0, :, cols(q)])

    def factors_coarse(s):
        factors(4 + s, 1, lambda q: coarse_rows(1 - s, 0, q))

    def w_copy(slot):
        return pltpu.make_async_remote_copy(
            src_ref=W.at[slot], dst_ref=W.at[slot], send_sem=w_send.at[slot], recv_sem=w_recv.at[slot],
            device_id=partner, device_id_type=pl.DeviceIdType.MESH,
        )

    def weights(slot, f, level):
        @pl.when(fld == 0)
        def _():
            source = jnp.where(jnp.full(shape, level) == 1, row & 1, row)

            def one(q, _):
                W[slot, q] = GG[slot, q] * rows_of(X[f, q], source)
                return 0

            lax.fori_loop(0, TILES, one, 0, unroll=8)
            w_copy(slot).start()

        @pl.when(fld == 1)
        def _():
            w_copy(slot).wait_recv()

    def halo_copy(slot, way):
        return pltpu.make_async_remote_copy(
            src_ref=HS.at[slot, way], dst_ref=HR.at[slot, way], send_sem=h_send.at[slot, way],
            recv_sem=h_recv.at[slot, way], device_id=at(1 if way == 0 else -1),
            device_id_type=pl.DeviceIdType.MESH,
        )

    def stencil_matrix():
        def one(r, _):
            source = r * ROWS * 2 + lax.broadcasted_iota(jnp.int32, (2 * ROWS, 2 * LANES), 0)
            target = lax.broadcasted_iota(jnp.int32, (2 * ROWS, 2 * LANES), 1)
            apart = jnp.abs(source - target)
            near = (apart == 16) | ((apart == 1) & ((source >> 4) == (target >> 4)))
            entry = jnp.where(near, 1.0, jnp.where(apart == 0, -6.0, 0.0))
            MX[pl.ds(pl.multiple_of(r * ROWS * 2, ROWS * 2), ROWS * 2), :] = entry.astype(jnp.bfloat16)
            return 0

        lax.fori_loop(0, 16, one, 0)

    def laplace(v, level, g4, g5, emit):
        idx = [NI[level * 6 + face] for face in range(4)]
        has = [NL[level * 6 + face] > 0 for face in range(4)]

        def ghost(x, face):
            return jnp.where(has[face], rows_of(x, idx[face]), zero)

        matrix = MX[...]
        planes = jnp.concatenate(
            [jnp.concatenate([v(2 * i + jh) for i in range(16)], axis=0) for jh in range(2)], axis=1
        )
        inner = None
        for piece in range(3):
            rounded = planes.astype(jnp.bfloat16)
            term = jnp.dot(rounded, matrix, preferred_element_type=jnp.float32)
            inner = term if inner is None else inner + term
            if piece < 2:
                planes = planes - rounded.astype(jnp.float32)

        for i in range(16):
            j_edge = [
                jnp.where(lane < 16, ghost(lane_roll(v(2 * i + 1), 16), 2), zero),
                jnp.where(lane >= 112, ghost(lane_roll(v(2 * i), -16), 3), zero),
            ]
            for jh in range(2):
                q = 2 * i + jh
                u, m = q // 16, q % 16
                i_less = v(q - 2) if i > 0 else ghost(v(30 + jh), 0)
                i_more = v(q + 2) if i < 15 else ghost(v(jh), 1)
                k_edge = jnp.where(kk == 15, lane_roll(g5[u], 15 - m), zero)
                k_edge = jnp.where(kk == 0, lane_roll(g4[u], -m), k_edge)
                plane = inner[i * ROWS : (i + 1) * ROWS, jh * LANES : (jh + 1) * LANES]
                emit(q, v(q), ((i_less + i_more) + (j_edge[jh] + k_edge)) + plane)

    def pack(v, k):
        packed = []
        for u in range(2):
            out = zero
            for m in range(16):
                out = jnp.where(kk == m, lane_roll(v(u * 16 + m), m - k), out)
            packed.append(out)
        return packed

    def begin(s, f, level):
        slot = s * 5 + f
        wslot = level * 4 + s
        rate = RT[f]
        share = SH[f]
        scaled = FM[f] > 0

        for q in range(TILES):
            X[f, q] = X[f, q] * jnp.where(scaled, FF[wslot, q], 1.0) + share * W[wslot, q]
        low = pack(lambda q: X[f, q], 0)
        high = pack(lambda q: X[f, q], 15)
        idx4, idx5 = NI[level * 6 + 4], NI[level * 6 + 5]
        has4, has5 = NL[level * 6 + 4] > 0, NL[level * 6 + 5] > 0
        g4 = [jnp.where(has4, rows_of(x, idx4), zero) for x in high]
        g5 = [jnp.where(has5, rows_of(x, idx5), zero) for x in low]

        def emit(q, x, total):
            FL[f, q] = rate * total

        laplace(lambda q: X[f, q], level, g4, g5, emit)
        low_first = pack(lambda q: FL[f, q], 0)
        high_first = pack(lambda q: FL[f, q], 15)
        for u in range(2):
            HS[slot, 0, u] = high[u]
            HS[slot, 0, 2 + u] = high_first[u]
            HS[slot, 1, u] = low[u]
            HS[slot, 1, 2 + u] = low_first[u]
        halo_copy(slot, 0).start()
        halo_copy(slot, 1).start()

    def finish(s, f, level):
        slot = s * 5 + f
        rate = RT[f]
        halo_copy(slot, 0).wait_recv()
        halo_copy(slot, 1).wait_recv()
        idx4, idx5 = NI[level * 6 + 4], NI[level * 6 + 5]
        has4, has5 = NL[level * 6 + 4] > 0, NL[level * 6 + 5] > 0
        far4, far5 = NR[level * 2] > 0, NR[level * 2 + 1] > 0
        r4, r5, g4, g5 = [], [], [], []
        for u in range(2):
            r4.append(jnp.where(far4, rate * rows_of(HR[slot, 0, u], idx4), zero))
            r5.append(jnp.where(far5, rate * rows_of(HR[slot, 1, u], idx5), zero))
        for u in range(2):
            low_first = HS[slot, 1, 2 + u] + r4[u]
            high_first = HS[slot, 0, 2 + u] + r5[u]
            far_low = rows_of(HR[slot, 0, 2 + u], idx4) + rate * HS[slot, 1, u]
            far_high = rows_of(HR[slot, 1, 2 + u], idx5) + rate * HS[slot, 0, u]
            g4.append(jnp.where(has4, rows_of(high_first, idx4), jnp.where(far4, far_low, zero)))
            g5.append(jnp.where(has5, rows_of(low_first, idx5), jnp.where(far5, far_high, zero)))
        for q in range(TILES):
            u, m = q // 16, q % 16
            gain = jnp.where(kk == 15, lane_roll(r5[u], 15 - m), zero)
            FL[f, q] = FL[f, q] + jnp.where(kk == 0, lane_roll(r4[u], -m), gain)
        half_rate = 0.5 * rate

        def emit(q, x, total):
            X[f, q] = X[f, q] + (x + half_rate * total)

        laplace(lambda q: FL[f, q], level, g4, g5, emit)

    send_octants(0)
    stencil_matrix()
    for copy in (*large, small[8]):
        copy.wait()

    def parts(s, _):
        part_fine(s)

        @pl.when(fld == 1)
        def _():
            mix_copy(s).start()

        return 0

    lax.fori_loop(0, 4, parts, 0)

    def parts_coarse(s, _):
        part_coarse(s)

        @pl.when(fld == 1)
        def _():
            mix_copy(4 + s).start()

        return 0

    lax.fori_loop(0, 2, parts_coarse, 0)
    mask_coarse()

    def fine(s, _):
        factors_fine(s)
        return 0

    def coarse(s, _):
        factors_coarse(s)
        return 0

    @pl.when(fld == 0)
    def _():
        lax.fori_loop(0, 2, fine, 0)
        lax.fori_loop(0, 1, coarse, 0)

    small[9].wait()
    wait_octants(0)

    def take_seed(f, _):
        add_octants(0, f, lambda q: seed_fine[f, :, q * LANES : (q + 1) * LANES])
        return 0

    lax.fori_loop(0, FIELDS, take_seed, 0)
    weights(0, 0, 0)
    weights(4, COARSE, 1)

    def start(f, _):
        begin(0, f, f // 4)
        return 0

    lax.fori_loop(0, FIELDS + 1, start, 0)

    @pl.when(fld == 0)
    def _():
        lax.fori_loop(2, 4, fine, 0)
        lax.fori_loop(1, 2, coarse, 0)

    def turn(t, _):
        late = jnp.where(t >= 5, 1, 0)
        s = late * (1 + (t - 5) // 4)
        f = jnp.where(t >= 5, lax.rem(t + 3, 4), t)
        level = f // 4
        finish(s, f, level)

        @pl.when(level == 1)
        def _():
            send_octants(1)
            mask_coarse()

        @pl.when((s == 1) & (level == 0))
        def _():
            @pl.when(f == 0)
            def _():
                wait_octants(1)

            add_octants(1, f, lambda q: X[f, q])

        @pl.when((f == 0) | (level == 1))
        def _():
            weights(level * 4 + s + 1, f, level)

        begin(s + 1, f, level)

        return 0

    lax.fori_loop(0, 13, turn, 0)

    def last(t, _):
        f = lax.rem(t + 4, 5)
        level = f // 4
        finish(3 - 2 * level, f, level)

        @pl.when(level == 0)
        def _():
            for q in range(TILES):
                out_fine[f, :, q * LANES : (q + 1) * LANES] = X[f, q]

        @pl.when(level == 1)
        def _():
            for q in range(TILES):
                for v in range(FIELDS):
                    out_coarse[v, :, q * LANES : (q + 1) * LANES] = X[COARSE, q, 2 * v : 2 * v + 2, :]

        return 0

    lax.fori_loop(0, 5, last, 0)

    for rslot in range(2):
        for d in range(1, LINKS):
            octant_copy(rslot, d).wait_send()
    for s in range(4):
        for f in range(5 if s < 2 else 4):
            for way in range(2):
                halo_copy(s * 5 + f, way).wait_send()

    @pl.when(fld == 0)
    def _():
        for slot in range(6):
            w_copy(slot).wait_send()

    @pl.when(fld == 1)
    def _():
        for slot in range(6):
            mix_copy(slot).wait_send()


def shards(*args):
    n = lax.axis_size("blk")
    seed_fine, seed_coarse = args[0], args[1]
    vmem = pl.BlockSpec(memory_space=pltpu.VMEM)
    hbm = pl.BlockSpec(memory_space=pltpu.HBM)
    tile = (ROWS, LANES)

    def buffer(*lead):
        return pltpu.VMEM((*lead, *tile), jnp.float32)

    def table(*lead):
        return pltpu.VMEM((*lead, *tile), jnp.int32)

    dma = pltpu.SemaphoreType.DMA
    return pl.pallas_call(
        functools.partial(kernel, n),
        out_shape=(
            pltpu.VMEM(seed_fine.shape, jnp.float32),
            pltpu.VMEM(seed_coarse.shape, jnp.float32),
        ),
        in_specs=[hbm] * 11,
        out_specs=(vmem, vmem),
        scratch_shapes=[
            *(pltpu.VMEM(x.shape, jnp.float32) for x in args[:4]),
            *(pltpu.SMEM(x.shape, x.dtype) for x in args[4:]),
            dma((14,)),
            pltpu.VMEM((2 * LANES, 2 * LANES), jnp.bfloat16),
            buffer(5, TILES), buffer(5, TILES),
            buffer(6, TILES), buffer(6, TILES), buffer(6, TILES), buffer(6, TILES), buffer(6, TILES),
            buffer(20, 2, 4), buffer(20, 2, 4),
            buffer(2, LINKS, 3), buffer(2, LINKS, 3),
            table(12), table(12), table(4),
            buffer(5), buffer(5), buffer(5), buffer(4), buffer(2), table(2),
            pltpu.SMEM((2 * LINKS,), jnp.int32),
            dma((20, 2)), dma((20, 2)), dma((6,)), dma((6,)), dma((6,)), dma((6,)), dma((2, LINKS)), dma((2, LINKS)),
        ],
        compiler_params=pltpu.CompilerParams(
            collective_id=0, has_side_effects=True, vmem_limit_bytes=62_000_000
        ),
    )(*args)


def solution(mesh):
    return jax.shard_map(
        shards,
        mesh=mesh,
        in_specs=(
            P("fld", "blk", None),
            P("fld", "blk", None),
            P(None, "fld", "blk", None),
            P(None, "fld", "blk", None),
            P("fld"),
            P("fld"),
            P("blk", None),
            P("blk", None),
            P("blk", None),
            P("blk"),
            P("blk"),
        ),
        out_specs=(P("fld", "blk", None), P("fld", "blk", None)),
        check_vma=False,
    )
```
